32 devices in a mesh: ctx: 8 (over z, x), head: 4 (over y, core).
Axes of the slice: x: 2, y: 2, z: 4, core: 2. Of those that a mesh axis runs over, the one named last changes fastest.
Arguments:
- queries: bfloat16 [2048, 8192], P('ctx', 'head'), may hold values from -20 to 20
- keys: bfloat16 [2048, 1024], P('ctx', 'head'), may hold values from -4 to 4
- values: bfloat16 [2048, 1024], P('ctx', 'head'), may hold values from -6 to 6
- grad_out: bfloat16 [2048, 8192], P('ctx', 'head'), may hold values from -6 to 6
- key_blocks: int32 [16, 6], replicated, may hold values from 0 to 15, as said below
- key_count: int32 [16], replicated, may hold values from 2 to 6
Outputs:
- attended: bfloat16 [2048, 8192], P('ctx', 'head')
- grad_q: bfloat16 [2048, 8192], P('ctx', 'head')
- grad_k: bfloat16 [2048, 1024], P('ctx', 'head')
- grad_v: bfloat16 [2048, 1024], P('ctx', 'head')
The draws below stay inside these ranges and needn't reach their ends.
Inputs may be any that keep to these rules, and one draw needn't show every extreme that they name: `key_blocks`: the listed key blocks of block b lie outside the range of 2 blocks that holds b (ranges begin at multiples of 2), each in a different range. Over the used slots of all query blocks of one range, at most 2 name blocks of any one other range; in every draw the query blocks of one range use all their 6 slots, so that this most and 12 used slots of one range are reached.
All inputs are finite; a program needn't handle non-finite values.
Results may differ from the reference program's by a relative error of at most 0.034.
Values may be sent and summed in bfloat16 or wider, within the bound.
No kernel may reach another device: no remote copies, remote signals or barrier semaphores. Data moves between devices by JAX's collectives and lax.ppermute only.
A program may use at most 64 MiB of HBM per device.

```python
import math
import jax
import jax.numpy as jnp
from jax import lax

QH = 64
KVH = 8
DH = 128
BLOCK = 128
KSLOTS = 6
BLK_DEV = 2
SEQ = 2048
N_CTX = 8


def draw_queries(key, part):
    result = jnp.clip(jax.random.normal(jax.random.fold_in(key, 1), (SEQ, QH * DH), jnp.float32), -4.0, 4.0)
    return result.astype(jnp.bfloat16)


def draw_keys(key, part):
    result = jnp.clip(jax.random.normal(jax.random.fold_in(key, 2), (SEQ, KVH * DH), jnp.float32), -4.0, 4.0)
    return result.astype(jnp.bfloat16)


def block_lists(key):
    base_key = jax.random.fold_in(key, 11)
    subkeys = jax.random.split(base_key, 5)
    entries = BLK_DEV * KSLOTS
    orders = jax.vmap(lambda subkey: jax.random.permutation(subkey, N_CTX - 1))(jax.random.split(subkeys[0], N_CTX))
    device = jnp.arange(N_CTX)[:, None]
    owner_ids = (device + 1 + orders[:, jnp.arange(entries) % (N_CTX - 1)]) % N_CTX
    within = jax.random.randint(subkeys[1], (N_CTX, entries), 0, BLK_DEV)
    blocks = (owner_ids * BLK_DEV + within).reshape(N_CTX * BLK_DEV, KSLOTS)
    cap_rows = jax.random.randint(subkeys[2], (N_CTX, 1), 3, KSLOTS + 1)
    counts = jax.random.randint(subkeys[3], (N_CTX, BLK_DEV), cap_rows - 1, cap_rows + 1)
    heavy_ctx = jax.random.randint(subkeys[4], (), 0, N_CTX)
    counts = jnp.where(device == heavy_ctx, KSLOTS, counts)
    return (blocks.astype(jnp.int32), counts.reshape(N_CTX * BLK_DEV).astype(jnp.int32))


def draw_key_blocks(key, part):
    return block_lists(key)[0]


def draw_key_count(key, part):
    return block_lists(key)[1]


def steps_of(stream_key, extent, pieces, low, top_value):
    def one(axis_at, parts):
        heights = jax.random.uniform(jax.random.fold_in(jax.random.fold_in(stream_key, 6), axis_at), (parts,), jnp.float32, low / len(pieces), top_value / len(pieces))
        return jnp.repeat(jnp.exp(heights), extent[axis_at] // parts).reshape((-1,) + (1,) * (len(extent) - axis_at - 1))

    level = one(*pieces[0])
    for cut in pieces[1:]:
        level = level * one(*cut)
    return level


def normal_values(own_key, shape, scale, reach, cuts=(), held_as=jnp.bfloat16):
    values = jax.random.normal(own_key, shape, jnp.float32) * scale
    if len(cuts) > 0:
        values = steps_of(own_key, shape, cuts, -0.22, 0.18) * values
    return jnp.clip(values, min=-reach, max=reach).astype(held_as)


def setup_inputs(seed: int = 0) -> dict:
    arg_keys = jax.random.split(jax.random.key(seed), 7)
    queries = draw_queries(jax.random.fold_in(arg_keys[6], 71), 0)
    keys = draw_keys(jax.random.fold_in(arg_keys[6], 71), 0)
    values = normal_values(arg_keys[2], (SEQ, KVH * DH), 1.0, 6.0, ((0, 8), (1, 4)))
    grad_out = normal_values(arg_keys[3], (SEQ, QH * DH), 1.0, 6.0, ((0, 8), (1, 4)))
    key_blocks = draw_key_blocks(jax.random.fold_in(arg_keys[6], 71), 0)
    key_count = draw_key_count(jax.random.fold_in(arg_keys[6], 71), 0)
    return dict(queries=queries, keys=keys, values=values, grad_out=grad_out, key_blocks=key_blocks, key_count=key_count)


def reference(queries, keys, values, grad_out, key_blocks, key_count):
    group_size = QH // KVH
    scaling = 1.0 / math.sqrt(DH)
    block_count = SEQ // BLOCK
    key_width = (KSLOTS + 1) * BLOCK
    query_tiles = queries.reshape(block_count, BLOCK, KVH, group_size, DH)
    grad_tiles = grad_out.reshape(block_count, BLOCK, KVH, group_size, DH)
    key_tiles = keys.reshape(block_count, BLOCK, KVH, DH)
    value_tiles = values.reshape(block_count, BLOCK, KVH, DH)
    slot_ids = jnp.arange(KSLOTS, dtype=jnp.int32)

    def visit_block(carried, block_id):
        sum_k, sum_v = carried
        chosen = jnp.concatenate([block_id.reshape(1).astype(jnp.int32), key_blocks[block_id].astype(jnp.int32)])
        is_live = jnp.concatenate([jnp.ones((1,), dtype=bool), slot_ids < key_count[block_id]])
        column = jnp.repeat(is_live, BLOCK)
        near_k = key_tiles[chosen].reshape(key_width, KVH, DH).astype(jnp.float32)
        near_v = value_tiles[chosen].reshape(key_width, KVH, DH).astype(jnp.float32)
        query_tile = query_tiles[block_id].astype(jnp.float32)
        grad_tile = grad_tiles[block_id].astype(jnp.float32)
        scores = jnp.einsum('qhgd,khd->hgqk', query_tile, near_k) * scaling
        scores = jnp.where(column, scores, -1e+30)
        row_max = lax.optimization_barrier(jnp.max(scores, axis=-1, keepdims=True))
        expo_terms = jnp.where(column, jnp.exp(scores - row_max), 0.0)
        prob_rows = expo_terms / lax.optimization_barrier(jnp.sum(expo_terms, axis=-1, keepdims=True))
        weights = lax.optimization_barrier(prob_rows.astype(jnp.bfloat16)).astype(jnp.float32)
        attended = jnp.einsum('hgqk,khd->qhgd', weights, near_v).astype(jnp.bfloat16)
        delta_rows = lax.optimization_barrier(jnp.sum(grad_tile * attended.astype(jnp.float32), axis=-1))
        grad_p = jnp.einsum('qhgd,khd->hgqk', grad_tile, near_v)
        grad_s = prob_rows * (grad_p - jnp.transpose(delta_rows, (1, 2, 0))[..., None]) * scaling
        grad_s = lax.optimization_barrier(grad_s.astype(jnp.bfloat16)).astype(jnp.float32)
        grad_q = jnp.einsum('hgqk,khd->qhgd', grad_s, near_k).astype(jnp.bfloat16)
        part_k = jnp.einsum('hgqk,qhgd->khd', grad_s, query_tile).reshape(KSLOTS + 1, BLOCK, KVH, DH)
        part_v = jnp.einsum('hgqk,qhgd->khd', weights, grad_tile).reshape(KSLOTS + 1, BLOCK, KVH, DH)
        sum_k = sum_k.at[chosen].add(part_k)
        sum_v = sum_v.at[chosen].add(part_v)
        return ((sum_k, sum_v), (attended, grad_q))
    start_sums = (jnp.zeros((block_count, BLOCK, KVH, DH), jnp.float32), jnp.zeros((block_count, BLOCK, KVH, DH), jnp.float32))
    (sum_k, sum_v), (attended, grad_q) = lax.scan(visit_block, start_sums, jnp.arange(block_count, dtype=jnp.int32))
    return (attended.reshape(SEQ, QH * DH), grad_q.reshape(SEQ, QH * DH), sum_k.astype(jnp.bfloat16).reshape(SEQ, KVH * DH), sum_v.astype(jnp.bfloat16).reshape(SEQ, KVH * DH))
```

```python
import functools
import math

import jax
import jax.numpy as jnp
from jax import lax
from jax.experimental import pallas as pl
from jax.experimental.pallas import tpu as pltpu
from jax.sharding import PartitionSpec as P

QH = 64
KVH = 8
DH = 128
BLOCK = 128
KSLOTS = 6

SCALE = 1.0 / math.sqrt(DH)
EXP2_SCALE = SCALE * math.log2(math.e)
DEAD = -1e30
VMEM_BYTES = 24 * 1024 * 1024

NT = (((1,), (1,)), ((), ()))


def dot(a, b):
    return jnp.dot(a, b, preferred_element_type=jnp.float32)


def dot_t(a, b):
    return lax.dot_general(a, b, NT, preferred_element_type=jnp.float32)


def params():
    return pltpu.CompilerParams(
        dimension_semantics=("arbitrary",), vmem_limit_bytes=VMEM_BYTES
    )


def cost(flops, size):
    return pl.CostEstimate(flops=int(flops), bytes_accessed=int(size), transcendentals=0)


def split3(x):
    hi = x.astype(jnp.bfloat16)
    rest = x - hi.astype(jnp.float32)
    mid = rest.astype(jnp.bfloat16)
    low = (rest - mid.astype(jnp.float32)).astype(jnp.bfloat16)
    return hi.astype(jnp.float32), mid.astype(jnp.float32), low.astype(jnp.float32)


def stat_lanes(x, last):
    lane = lax.broadcasted_iota(jnp.int32, x.shape, 1)
    hi, mid, low = split3(x)
    tail = jnp.where(lane == 3, last, 0.0)
    return jnp.where(
        lane == 0, hi, jnp.where(lane == 1, mid, jnp.where(lane == 2, low, tail))
    ).astype(jnp.bfloat16)


def key_lanes(rows, bias):
    lane = lax.broadcasted_iota(jnp.int32, (rows, DH), 1)
    return jnp.where(lane < 3, 1.0, jnp.where(lane == 3, bias, 0.0)).astype(jnp.bfloat16)


def pick(ref, w, offset):
    return ref[pl.ds(pl.multiple_of(offset + jnp.maximum(w, 0) * BLOCK, BLOCK), BLOCK), :]


def bias_of(w):
    return jnp.where(w >= 0, 0.0, DEAD)


def prep_kernel(group, q_ref, o_ref, qp_ref, op_ref, qt_ref, ot_ref):
    for g in range(group):
        cols = slice(g * DH, (g + 1) * DH)
        rows = slice(g * BLOCK, (g + 1) * BLOCK)
        for src, dst, dst_t in ((q_ref, qp_ref, qt_ref), (o_ref, op_ref, ot_ref)):
            tile = src[:, cols]
            dst[0, rows, :] = tile
            dst_t[0, :, rows] = tile.T


def prep(q, o, combos, heads, group):
    rows = group * BLOCK
    wide = pl.BlockSpec((BLOCK, group * DH), lambda c: (c // heads, c % heads))
    tall = pl.BlockSpec((1, rows, DH), lambda c: (c, 0, 0))
    flat = pl.BlockSpec((1, DH, rows), lambda c: (c, 0, 0))
    return pl.pallas_call(
        functools.partial(prep_kernel, group),
        grid=(combos,),
        in_specs=[wide, wide],
        out_specs=[tall, tall, flat, flat],
        out_shape=[jax.ShapeDtypeStruct((combos, rows, DH), jnp.bfloat16)] * 2
        + [jax.ShapeDtypeStruct((combos, DH, rows), jnp.bfloat16)] * 2,
        compiler_params=params(),
        cost_estimate=cost(1e9, 6 * q.size * 2),
        name="prep",
    )(q, o)


def forward_kernel(heads, offsets, tile, tbl, q_ref, ko_ref, vo_ref, *refs):
    kv_refs = refs[: len(offsets)]
    out_ref, lse_ref, k_scr, v_scr = refs[len(offsets) :]
    b = pl.program_id(0) // heads
    width = k_scr.shape[0]
    k_scr[0:BLOCK, :] = ko_ref[...]
    v_scr[0:BLOCK, :] = vo_ref[...]
    biases = [jnp.zeros((1, BLOCK), jnp.float32)]
    for i, (ref, j) in enumerate(zip(kv_refs, offsets)):
        w = tbl[b, j]
        dst = slice((i + 1) * BLOCK, (i + 2) * BLOCK)
        k_scr[dst, :] = pick(ref, w, 0)
        v_scr[dst, :] = pick(ref, w, ref.shape[0] // 2)
        biases.append(jnp.full((1, BLOCK), bias_of(w), jnp.float32))
    bias = jnp.concatenate(biases, axis=1)

    def step(t, carry):
        rows = pl.ds(pl.multiple_of(t * tile, tile), tile)
        x = dot_t(q_ref[0, rows, :], k_scr[...]) * EXP2_SCALE + bias
        m = jnp.max(x, axis=1, keepdims=True)
        p = jnp.exp2(x - m)
        total = jnp.sum(p, axis=1, keepdims=True)
        out_ref[0, rows, :] = dot(p.astype(jnp.bfloat16), v_scr[...]) / total
        lse_ref[0, rows, :] = jnp.broadcast_to(m + jnp.log2(total), (tile, DH))
        return carry

    lax.fori_loop(0, q_ref.shape[1] // tile, step, 0, unroll=2)


def forward(tbl, qp, k, v, kvs, offsets, heads):
    combos, rows, _ = qp.shape
    width = (len(kvs) + 1) * BLOCK
    tall = pl.BlockSpec((1, rows, DH), lambda c, t: (c, 0, 0))
    own = pl.BlockSpec((BLOCK, DH), lambda c, t: (c // heads, c % heads))
    far = [pl.BlockSpec((a.shape[0], DH), lambda c, t: (0, c % heads)) for a in kvs]
    return pl.pallas_call(
        functools.partial(forward_kernel, heads, offsets, 128),
        grid_spec=pltpu.PrefetchScalarGridSpec(
            num_scalar_prefetch=1,
            grid=(combos,),
            in_specs=[tall, own, own] + far,
            out_specs=[tall, tall],
            scratch_shapes=[pltpu.VMEM((width, DH), jnp.bfloat16)] * 2,
        ),
        out_shape=[jax.ShapeDtypeStruct((combos, rows, DH), jnp.float32)] * 2,
        compiler_params=params(),
        cost_estimate=cost(4 * combos * rows * width * DH, combos * rows * DH * 10),
        name="forward",
    )(tbl, qp, k, v, *kvs)


def turn_kernel(
    heads, opposite, tile, tbl, q_ref, o_ref, qt_ref, ot_ref, k_ref, v_ref, out1_ref, lse1_ref,
    att_ref, sq_ref, so_ref, ds_ref, pk_ref, pv_ref, w_scr,
):
    c = pl.program_id(0)
    b, h = c // heads, c % heads
    w = tbl[b, opposite]
    k4 = pick(k_ref, w, 0)
    v4 = pick(v_ref, w, 0)
    bias = bias_of(w)

    @pl.when(c == 0)
    def _():
        pk_ref[...] = jnp.zeros_like(pk_ref)
        pv_ref[...] = jnp.zeros_like(pv_ref)

    for t in range(q_ref.shape[1] // tile):
        rows = slice(t * tile, (t + 1) * tile)
        x = dot_t(q_ref[0, rows, :], k4) * EXP2_SCALE + bias
        grad_p = dot_t(o_ref[0, rows, :], v4)
        lse1 = lse1_ref[0, rows, :]
        m = jnp.maximum(lse1, jnp.max(x, axis=1, keepdims=True))
        p = jnp.exp2(x - m)
        a = jnp.exp2(lse1 - m)
        total = a + jnp.sum(p, axis=1, keepdims=True)
        inverse = 1.0 / total
        p = p * inverse
        weights = p.astype(jnp.bfloat16)
        att = (out1_ref[0, rows, :] * (a * inverse) + dot(weights, v4)).astype(jnp.bfloat16)
        for g in range(tile // BLOCK):
            att_ref[:, t * tile + g * DH : t * tile + (g + 1) * DH] = att[
                g * BLOCK : (g + 1) * BLOCK, :
            ]
        delta = jnp.sum(
            o_ref[0, rows, :].astype(jnp.float32) * att.astype(jnp.float32), axis=1, keepdims=True
        )
        ds_ref[0, rows, :] = (p * ((grad_p - delta) * SCALE)).astype(jnp.bfloat16)
        w_scr[rows, :] = weights
        sq_ref[0, rows, :] = stat_lanes((m + jnp.log2(total)) * (-1.0 / EXP2_SCALE), 1.0)
        so_ref[0, rows, :] = stat_lanes(jnp.broadcast_to(-delta, (tile, DH)), 0.0)

    lanes = pl.ds(pl.multiple_of(jnp.maximum(w, 0) * BLOCK, BLOCK), BLOCK)
    head_rows = pl.ds(pl.multiple_of(h * DH, DH), DH)
    pk_ref[head_rows, lanes] += dot(qt_ref[0], ds_ref[0])
    pv_ref[head_rows, lanes] += dot(ot_ref[0], w_scr[...])


def turn(tbl, qp, op, qt, ot, k4, v4, out1, lse1, opposite, heads, q_shape):
    combos, rows, _ = qp.shape
    own_rows = k4.shape[0]
    group = rows // BLOCK
    tall = pl.BlockSpec((1, rows, DH), lambda c, t: (c, 0, 0))
    flat = pl.BlockSpec((1, DH, rows), lambda c, t: (c, 0, 0))
    far = pl.BlockSpec((own_rows, DH), lambda c, t: (0, c % heads))
    wide = pl.BlockSpec((BLOCK, group * DH), lambda c, t: (c // heads, c % heads))
    part = pl.BlockSpec((heads * DH, own_rows), lambda c, t: (0, 0))
    slab = jax.ShapeDtypeStruct((combos, rows, DH), jnp.bfloat16)
    return pl.pallas_call(
        functools.partial(turn_kernel, heads, opposite, 256),
        grid_spec=pltpu.PrefetchScalarGridSpec(
            num_scalar_prefetch=1,
            grid=(combos,),
            in_specs=[tall, tall, flat, flat, far, far, tall, tall],
            out_specs=[wide, tall, tall, tall, part, part],
            scratch_shapes=[pltpu.VMEM((rows, DH), jnp.bfloat16)],
        ),
        out_shape=[jax.ShapeDtypeStruct(q_shape, jnp.bfloat16), slab, slab, slab]
        + [jax.ShapeDtypeStruct((heads * DH, own_rows), jnp.float32)] * 2,
        compiler_params=params(),
        cost_estimate=cost(10 * combos * rows * BLOCK * DH, combos * rows * DH * 20),
        name="turn",
    )(tbl, qp, op, qt, ot, k4, v4, out1, lse1)


def pair_grads(q_ref, sq_ref, o_ref, so_ref, k, v, lanes_k, lanes_v, ds_ref, w_scr, tile):
    key = jnp.concatenate([k, lanes_k], axis=1)
    value = jnp.concatenate([v, lanes_v], axis=1)
    for t in range(q_ref.shape[1] // tile):
        rows = slice(t * tile, (t + 1) * tile)
        x = dot_t(jnp.concatenate([q_ref[0, rows, :], sq_ref[0, rows, :]], axis=1), key)
        d = dot_t(jnp.concatenate([o_ref[0, rows, :], so_ref[0, rows, :]], axis=1), value)
        p = jnp.exp2(x * EXP2_SCALE)
        w_scr[rows, :] = p.astype(jnp.bfloat16)
        ds_ref[rows, :] = (p * (d * SCALE)).astype(jnp.bfloat16)


def back_kernel(
    heads, ahead, behind, tile, tbl, q_ref, sq_ref, o_ref, so_ref, qt_ref, ot_ref, a_ref, b_ref,
    pa_ref, pb_ref, ds_ref, w_scr,
):
    c = pl.program_id(0)
    b, h = c // heads, c % heads
    wa, wb = tbl[b, ahead], tbl[b, behind]
    half = a_ref.shape[0] // 2
    k = jnp.concatenate([pick(a_ref, wa, 0), pick(b_ref, wb, 0)], axis=0)
    v = jnp.concatenate([pick(a_ref, wa, half), pick(b_ref, wb, half)], axis=0)
    lanes_k = jnp.concatenate(
        [key_lanes(BLOCK, bias_of(wa)), key_lanes(BLOCK, bias_of(wb))], axis=0
    )

    @pl.when(c == 0)
    def _():
        pa_ref[...] = jnp.zeros_like(pa_ref)
        pb_ref[...] = jnp.zeros_like(pb_ref)

    pair_grads(
        q_ref, sq_ref, o_ref, so_ref, k, v, lanes_k, key_lanes(2 * BLOCK, 0.0),
        ds_ref.at[0], w_scr, tile,
    )
    dk = dot(qt_ref[0], ds_ref[0])
    dv = dot(ot_ref[0], w_scr[...])
    for i, (ref, w) in enumerate(((pa_ref, wa), (pb_ref, wb))):
        lanes = pl.ds(pl.multiple_of(jnp.maximum(w, 0) * BLOCK, BLOCK), BLOCK)
        src = slice(i * BLOCK, (i + 1) * BLOCK)
        ref[pl.ds(pl.multiple_of(h * DH, DH), DH), lanes] += dk[:, src]
        ref[pl.ds(pl.multiple_of((heads + h) * DH, DH), DH), lanes] += dv[:, src]


def back(tbl, qp, sq, op, so, qt, ot, kv_ahead, kv_behind, ahead, behind, heads):
    combos, rows, _ = qp.shape
    own_rows = kv_ahead.shape[0] // 2
    tall = pl.BlockSpec((1, rows, DH), lambda c, t: (c, 0, 0))
    flat = pl.BlockSpec((1, DH, rows), lambda c, t: (c, 0, 0))
    far = pl.BlockSpec((2 * own_rows, DH), lambda c, t: (0, c % heads))
    part = pl.BlockSpec((2 * heads * DH, own_rows), lambda c, t: (0, 0))
    return pl.pallas_call(
        functools.partial(back_kernel, heads, ahead, behind, 256),
        grid_spec=pltpu.PrefetchScalarGridSpec(
            num_scalar_prefetch=1,
            grid=(combos,),
            in_specs=[tall, tall, tall, tall, flat, flat, far, far],
            out_specs=[part, part, pl.BlockSpec((1, rows, 2 * BLOCK), lambda c, t: (c, 0, 0))],
            scratch_shapes=[pltpu.VMEM((rows, 2 * BLOCK), jnp.bfloat16)],
        ),
        out_shape=[jax.ShapeDtypeStruct((2 * heads * DH, own_rows), jnp.float32)] * 2
        + [jax.ShapeDtypeStruct((combos, rows, 2 * BLOCK), jnp.bfloat16)],
        compiler_params=params(),
        cost_estimate=cost(16 * combos * rows * BLOCK * DH, combos * rows * DH * 16),
        name="back",
    )(tbl, qp, sq, op, so, qt, ot, kv_ahead, kv_behind)


def own_kernel(
    heads, opposite, pairs, tile, tbl, q_ref, sq_ref, o_ref, so_ref, qt_ref, ot_ref, k_ref, v_ref,
    k4_ref, ds4_ref, *refs,
):
    far = refs[: 3 * len(pairs)]
    gq_ref, part_ref, ds_scr, w_scr, k_scr = refs[3 * len(pairs) :]
    c = pl.program_id(0)
    b, h = c // heads, c % heads
    pair_grads(
        q_ref, sq_ref, o_ref, so_ref, k_ref[...], v_ref[...], key_lanes(BLOCK, 0.0),
        key_lanes(BLOCK, 0.0), ds_scr, w_scr, tile,
    )
    lanes = pl.ds(pl.multiple_of(b * BLOCK, BLOCK), BLOCK)
    part_ref[pl.ds(pl.multiple_of(h * DH, DH), DH), lanes] = dot(qt_ref[0], ds_scr[...])
    part_ref[pl.ds(pl.multiple_of((heads + h) * DH, DH), DH), lanes] = dot(ot_ref[0], w_scr[...])
    k_scr[0:BLOCK, :] = k_ref[...]
    k_scr[BLOCK : 2 * BLOCK, :] = pick(k4_ref, tbl[b, opposite], 0)
    for i, (ahead, behind) in enumerate(pairs):
        base = (2 + 2 * i) * BLOCK
        k_scr[base : base + BLOCK, :] = pick(far[3 * i], tbl[b, ahead], 0)
        k_scr[base + BLOCK : base + 2 * BLOCK, :] = pick(far[3 * i + 1], tbl[b, behind], 0)
    for t in range(q_ref.shape[1] // tile):
        rows = slice(t * tile, (t + 1) * tile)
        total = dot(
            jnp.concatenate([ds_scr[rows, :], ds4_ref[0, rows, :]], axis=1), k_scr[0 : 2 * BLOCK, :]
        )
        for i in range(len(pairs)):
            base = (2 + 2 * i) * BLOCK
            total += dot(far[3 * i + 2][0, rows, :], k_scr[base : base + 2 * BLOCK, :])
        total = total.astype(jnp.bfloat16)
        for g in range(tile // BLOCK):
            gq_ref[:, t * tile + g * DH : t * tile + (g + 1) * DH] = total[
                g * BLOCK : (g + 1) * BLOCK, :
            ]


def own_grads(tbl, qp, sq, op, so, qt, ot, k, v, k4, ds4, far, pairs, opposite, heads, q_shape):
    combos, rows, _ = qp.shape
    own_rows = k.shape[0]
    group = rows // BLOCK
    tall = pl.BlockSpec((1, rows, DH), lambda c, t: (c, 0, 0))
    flat = pl.BlockSpec((1, DH, rows), lambda c, t: (c, 0, 0))
    own = pl.BlockSpec((BLOCK, DH), lambda c, t: (c // heads, c % heads))
    side = pl.BlockSpec((own_rows, DH), lambda c, t: (0, c % heads))
    wide = pl.BlockSpec((BLOCK, group * DH), lambda c, t: (c // heads, c % heads))
    pair = pl.BlockSpec((1, rows, 2 * BLOCK), lambda c, t: (c, 0, 0))
    part = pl.BlockSpec((2 * heads * DH, own_rows), lambda c, t: (0, 0))
    return pl.pallas_call(
        functools.partial(own_kernel, heads, opposite, pairs, 256),
        grid_spec=pltpu.PrefetchScalarGridSpec(
            num_scalar_prefetch=1,
            grid=(combos,),
            in_specs=[tall, tall, tall, tall, flat, flat, own, own, side, tall]
            + [side, side, pair] * len(pairs),
            out_specs=[wide, part],
            scratch_shapes=[
                pltpu.VMEM((rows, BLOCK), jnp.bfloat16),
                pltpu.VMEM((rows, BLOCK), jnp.bfloat16),
                pltpu.VMEM(((2 + 2 * len(pairs)) * BLOCK, DH), jnp.bfloat16),
            ],
        ),
        out_shape=[
            jax.ShapeDtypeStruct(q_shape, jnp.bfloat16),
            jax.ShapeDtypeStruct((2 * heads * DH, own_rows), jnp.float32),
        ],
        compiler_params=params(),
        cost_estimate=cost(
            (10 + 4 * len(pairs)) * combos * rows * BLOCK * DH, combos * rows * DH * 20
        ),
        name="own_grads",
    )(tbl, qp, sq, op, so, qt, ot, k, v, k4, ds4, *far)


def finish_kernel(own_ref, a_ref, b_ref, gk_ref, gv_ref):
    total = own_ref[...] + (a_ref[...].astype(jnp.float32) + b_ref[...].astype(jnp.float32))
    half = total.shape[0] // 2
    gk_ref[...] = total[:half, :].T.astype(jnp.bfloat16)
    gv_ref[...] = total[half:, :].T.astype(jnp.bfloat16)


def finish(own_part, from_behind, from_ahead):
    size, rows = own_part.shape
    return pl.pallas_call(
        finish_kernel,
        out_shape=[jax.ShapeDtypeStruct((rows, size // 2), jnp.bfloat16)] * 2,
        compiler_params=pltpu.CompilerParams(vmem_limit_bytes=VMEM_BYTES),
        cost_estimate=cost(1e7, own_part.size * 10),
        name="finish",
    )(own_part, from_behind, from_ahead)


def local(queries, keys, values, grad_out, key_blocks, key_count):
    n = lax.axis_size("ctx")
    me = lax.axis_index("ctx")
    row_count, width = keys.shape
    blk_dev = row_count // BLOCK
    heads = width // DH
    group = QH // KVH
    combos = blk_dev * heads
    opposite = n // 2
    steps = opposite - 1

    order = list(range(0, n, 2)) + list(range(n - 1, 0, -2))
    up = [(order[i], order[(i + 1) % n]) for i in range(n)]
    down = [(b, a) for a, b in up]

    def place(index):
        return jnp.where(index % 2 == 0, index // 2, n - 1 - index // 2)

    blocks = lax.dynamic_slice_in_dim(key_blocks, me * blk_dev, blk_dev, 0)
    counts = lax.dynamic_slice_in_dim(key_count, me * blk_dev, blk_dev, 0)
    live = jnp.arange(blocks.shape[1])[None, :] < counts[:, None]
    offset = (place(blocks // blk_dev) - place(me) + n) % n
    hit = live[:, :, None] & (offset[:, :, None] == jnp.arange(n)[None, None, :])
    tbl = jnp.sum(jnp.where(hit, (blocks % blk_dev)[:, :, None] + 1, 0), axis=1) - 1

    kv = jnp.concatenate([keys, values], axis=0)
    behind, ahead = [kv], [kv]
    for _ in range(steps):
        behind.append(lax.ppermute(behind[-1], "ctx", up))
        ahead.append(lax.ppermute(ahead[-1], "ctx", down))
    k4 = lax.ppermute(behind[-1][:row_count], "ctx", up)
    v4 = lax.ppermute(ahead[-1][row_count:], "ctx", down)

    qp, op, qt, ot = prep(queries, grad_out, combos, heads, group)
    kvs, offsets = [], []
    for s in range(1, steps + 1):
        kvs += [ahead[s], behind[s]]
        offsets += [s, n - s]
    out1, lse1 = forward(tbl, qp, keys, values, kvs, tuple(offsets), heads)
    attended, sq, so, ds4, pk, pv = turn(
        tbl, qp, op, qt, ot, k4, v4, out1, lse1, opposite, heads, queries.shape
    )

    up_in = lax.ppermute(pk.astype(jnp.bfloat16), "ctx", up)
    down_in = lax.ppermute(pv.astype(jnp.bfloat16), "ctx", down)
    half = heads * DH
    far = {}
    for s in range(steps, 0, -1):
        part_a, part_b, ds = back(
            tbl, qp, sq, op, so, qt, ot, ahead[s], behind[s], s, n - s, heads
        )
        far[s] = (ahead[s], behind[s], ds)
        if s == steps:
            up_out = jnp.concatenate([part_a[:half] + up_in.astype(jnp.float32), part_a[half:]])
            down_out = jnp.concatenate([part_b[:half], part_b[half:] + down_in.astype(jnp.float32)])
        else:
            up_out = part_a + up_in.astype(jnp.float32)
            down_out = part_b + down_in.astype(jnp.float32)
        up_in = lax.ppermute(up_out.astype(jnp.bfloat16), "ctx", up)
        down_in = lax.ppermute(down_out.astype(jnp.bfloat16), "ctx", down)
    pairs = tuple((s, n - s) for s in sorted(far))
    grad_q, own_part = own_grads(
        tbl, qp, sq, op, so, qt, ot, keys, values, k4, ds4,
        [a for s in sorted(far) for a in far[s]], pairs, opposite, heads, queries.shape,
    )
    grad_k, grad_v = finish(own_part, up_in, down_in)
    return attended, grad_q, grad_k, grad_v


def solution(mesh):
    spec = P("ctx", "head")
    return jax.shard_map(
        local,
        mesh=mesh,
        in_specs=(spec, spec, spec, spec, P(), P()),
        out_specs=(spec,) * 4,
        check_vma=False,
    )
```

```python
import functools
import math

import jax
import jax.numpy as jnp
from jax import lax
from jax.experimental import pallas as pl
from jax.experimental.pallas import tpu as pltpu
from jax.sharding import PartitionSpec as P


QH = 64
KVH = 8
DH = 128
BLOCK = 128

SCALE = 1.0 / math.sqrt(DH)
EXP2_SCALE = SCALE * math.log2(math.e)
FIRST_TILE = 512
NEAR_TILE = 512
TURN_TILE = 512
BACK_TILE = 512
NEAR_UNROLL = 1
TURN_UNROLL = 1
BACK_UNROLL = 1
VMEM_BYTES = 24 * 1024 * 1024

NT = (((1,), (1,)), ((), ()))
VMEM = pl.BlockSpec(memory_space=pltpu.VMEM)
SMEM = pl.BlockSpec(memory_space=pltpu.SMEM)
HBM = pl.BlockSpec(memory_space=pltpu.HBM)


def dot(a, b):
    return jnp.dot(a, b, preferred_element_type=jnp.float32)


def dot_t(a, b):
    return lax.dot_general(a, b, NT, preferred_element_type=jnp.float32)


def bf16(shape):
    return jax.ShapeDtypeStruct(shape, jnp.bfloat16)


def f32(shape):
    return jax.ShapeDtypeStruct(shape, jnp.float32)


def call(kernel, in_specs, out_shape, flops, args, scratch=(), out_specs=None):
    return pl.pallas_call(
        kernel,
        in_specs=in_specs,
        out_specs=out_specs or [VMEM] * len(out_shape),
        out_shape=out_shape,
        scratch_shapes=list(scratch),
        compiler_params=pltpu.CompilerParams(vmem_limit_bytes=VMEM_BYTES),
        cost_estimate=pl.CostEstimate(
            flops=int(flops), bytes_accessed=1 << 20, transcendentals=0
        ),
    )(*args)


def at(index, size):
    return pl.ds(pl.multiple_of(index * size, size), size)


def slot(w):
    return jnp.maximum(w, 0)


def block_of(ref, w, h, base=0):
    start = pl.multiple_of(base + slot(w) * BLOCK, BLOCK)
    return ref[pl.ds(start, BLOCK), at(h, DH)]


def key_of(ref, w, h, own):
    return jnp.where(w >= 0, block_of(ref, w, h), own)


def keep(w, x):
    return jnp.where(w >= 0, x, jnp.zeros_like(x))


def value_and_one(v, w):
    return keep(w, jnp.concatenate([v, jnp.ones_like(v)], axis=1))


def rows_of(*blocks):
    return jnp.concatenate(blocks, axis=0)


def tiles(rows, size):
    return [slice(t, t + size) for t in range(0, rows, size)]


def copies_of(src, dst, sems):
    copies = [pltpu.make_async_copy(s, d, sems.at[i]) for i, (s, d) in enumerate(zip(src, dst))]
    for c in copies:
        c.start()
    return copies


def pack_kernel(k_ref, v_ref, kv_ref, sems):
    rows = k_ref.shape[0]
    halves = [kv_ref.at[pl.ds(0, rows)], kv_ref.at[pl.ds(rows, rows)]]
    for c in copies_of([k_ref, v_ref], halves, sems):
        c.wait()


def first_kernel(heads, q_in, o_in, kv_ref, q_ref, o_ref, qt_ref, ot_ref, acc_ref, m_ref, sems):
    combos, rows, _ = q_ref.shape
    group = rows // BLOCK
    half = kv_ref.shape[0] // 2
    for c in range(combos):
        b, h = c // heads, c % heads
        for g in range(group):
            src = (pl.ds(b * BLOCK, BLOCK), pl.ds((h * group + g) * DH, DH))
            dst = pl.ds(g * BLOCK, BLOCK)
            pltpu.make_async_copy(q_in.at[src], q_ref.at[c, dst], sems.at[0, c]).start()
            pltpu.make_async_copy(o_in.at[src], o_ref.at[c, dst], sems.at[1, c]).start()

    def combo(c, carry):
        b, h = c // heads, c % heads
        pltpu.make_async_copy(q_ref.at[c], q_ref.at[c], sems.at[0, c]).wait()
        k = block_of(kv_ref, b, h)
        v = value_and_one(block_of(kv_ref, b, h, half), 0)
        for part in tiles(rows, FIRST_TILE):
            x = dot_t(q_ref[c, part, :], k) * EXP2_SCALE
            m = jnp.max(x, axis=1, keepdims=True)
            p = jnp.exp2(x - m)
            m_ref[c, part, :] = jnp.broadcast_to(m, x.shape)
            acc_ref[c, part, :] = dot(p.astype(jnp.bfloat16), v)
        pltpu.make_async_copy(o_ref.at[c], o_ref.at[c], sems.at[1, c]).wait()
        for src, dst in ((q_ref, qt_ref), (o_ref, ot_ref)):
            for part in tiles(rows, BLOCK):
                dst[c, :, part] = src[c, part, :].T
        return carry

    lax.fori_loop(0, combos, combo, 0)


def first(q, o, kv, combos, heads, group):
    rows = group * BLOCK
    return call(
        functools.partial(first_kernel, heads),
        [HBM] * 2 + [VMEM],
        [bf16((combos, rows, DH))] * 2
        + [bf16((combos, DH, rows))] * 2
        + [f32((combos, rows, 2 * DH)), f32((combos, rows, DH))],
        6 * combos * rows * BLOCK * DH,
        (q, o, kv),
        [pltpu.SemaphoreType.DMA((2, combos))],
    )


def near_kernel(
    heads, ja, jb, tbl, q_ref, kv_ref, a_ref, b_ref, acc_in, m_in, acc_ref, m_ref
):
    combos, rows, _ = q_ref.shape
    half = a_ref.shape[0] // 2

    def combo(c, carry):
        b, h = c // heads, c % heads
        wa, wb = tbl[b, ja], tbl[b, jb]
        own = block_of(kv_ref, b, h)
        k = rows_of(key_of(a_ref, wa, h, own), key_of(b_ref, wb, h, own))
        v = rows_of(
            value_and_one(block_of(a_ref, wa, h, half), wa),
            value_and_one(block_of(b_ref, wb, h, half), wb),
        )
        for part in tiles(rows, NEAR_TILE):
            x = dot_t(q_ref[c, part, :], k) * EXP2_SCALE
            old = m_in[c, part, :]
            m = jnp.maximum(old, jnp.max(x, axis=1, keepdims=True))
            a = jnp.exp2(old - m)
            p = jnp.exp2(x - jnp.concatenate([m, m], axis=1))
            m_ref[c, part, :] = m
            acc = acc_in[c, part, :] * jnp.concatenate([a, a], axis=1)
            acc_ref[c, part, :] = acc + dot(p.astype(jnp.bfloat16), v)
        return carry

    lax.fori_loop(0, combos, combo, 0, unroll=NEAR_UNROLL)


def near(tbl, q, kv, a, b, state, ja, jb, heads):
    combos, rows, _ = q.shape
    return call(
        functools.partial(near_kernel, heads, ja, jb),
        [SMEM] + [VMEM] * 6,
        [f32((combos, rows, 2 * DH)), f32((combos, rows, DH))],
        8 * combos * rows * BLOCK * DH,
        (tbl, q, kv, a, b, *state),
    )


def turn_kernel(
    heads, opposite, tbl, q_ref, o_ref, qt_ref, ot_ref, kv_ref, k_ref, v_ref, acc_in, m_in,
    att_ref, lse_ref, delta_ref, ds_ref, pk_ref, pv_ref, w_scr, pk_scr, pv_scr,
):
    combos, rows, _ = q_ref.shape
    pk_scr[...] = jnp.zeros_like(pk_scr)
    pv_scr[...] = jnp.zeros_like(pv_scr)

    def combo(c, carry):
        b, h = c // heads, c % heads
        w = tbl[b, opposite]
        k4 = key_of(k_ref, w, h, block_of(kv_ref, b, h))
        v4 = block_of(v_ref, w, h)
        v_one = value_and_one(v4, w)
        for part in tiles(rows, TURN_TILE):
            x = dot_t(q_ref[c, part, :], k4) * EXP2_SCALE
            grad_p = dot_t(o_ref[c, part, :], v4)
            old = m_in[c, part, :]
            m = jnp.maximum(old, jnp.max(x, axis=1, keepdims=True))
            a = jnp.exp2(old - m)
            p = jnp.exp2(x - m)
            acc = acc_in[c, part, :] * jnp.concatenate([a, a], axis=1)
            acc = acc + dot(p.astype(jnp.bfloat16), v_one)
            total = acc[:, DH:]
            inverse = 1.0 / total
            att = (acc[:, :DH] * inverse).astype(jnp.bfloat16)
            att_ref[c, part, :] = att
            delta = jnp.sum(
                o_ref[c, part, :].astype(jnp.float32) * att.astype(jnp.float32),
                axis=1,
                keepdims=True,
            )
            p = p * inverse
            w_scr[part, :] = p.astype(jnp.bfloat16)
            ds_ref[c, part, :] = (p * (grad_p - delta)).astype(jnp.bfloat16)
            lse_ref[c, part, :] = m + jnp.log2(total)
            delta_ref[c, part, :] = jnp.broadcast_to(delta, x.shape)
        pk_scr[at(h, DH), at(slot(w), BLOCK)] += keep(w, dot(qt_ref[c], ds_ref[c]))
        pv_scr[at(h, DH), at(slot(w), BLOCK)] += keep(w, dot(ot_ref[c], w_scr[...]))
        return carry

    lax.fori_loop(0, combos, combo, 0, unroll=TURN_UNROLL)
    pk_ref[...] = pk_scr[...].astype(jnp.bfloat16)
    pv_ref[...] = pv_scr[...].astype(jnp.bfloat16)


def turn(tbl, slabs, kv, k4, v4, state, opposite, heads):
    combos, rows, _ = slabs[0].shape
    own_rows = k4.shape[0]
    shape = (combos, rows, DH)
    return call(
        functools.partial(turn_kernel, heads, opposite),
        [SMEM] + [VMEM] * 9,
        [bf16(shape), f32(shape), f32(shape), bf16(shape)] + [bf16((heads * DH, own_rows))] * 2,
        10 * combos * rows * BLOCK * DH,
        (tbl, *slabs, kv, k4, v4, *state),
        [pltpu.VMEM((rows, DH), jnp.bfloat16)]
        + [pltpu.VMEM((heads * DH, own_rows), jnp.float32)] * 2,
    )


def weights_and_grads(c, q_ref, o_ref, lse_ref, delta_ref, k, v, ds_scr, w_scr):
    repeat = k.shape[0] // BLOCK
    for part in tiles(q_ref.shape[1], BACK_TILE):
        lse = jnp.concatenate([lse_ref[c, part, :]] * repeat, axis=1)
        delta = jnp.concatenate([delta_ref[c, part, :]] * repeat, axis=1)
        p = jnp.exp2(dot_t(q_ref[c, part, :], k) * EXP2_SCALE - lse)
        w_scr[part, :] = p.astype(jnp.bfloat16)
        ds_scr[part, :] = (p * (dot_t(o_ref[c, part, :], v) - delta)).astype(jnp.bfloat16)


def back_kernel(
    heads, ja, jb, has_sum, tbl, q_ref, o_ref, qt_ref, ot_ref, kv_ref, lse_ref, delta_ref, a_ref,
    b_ref, *refs,
):
    if has_sum:
        gq_in, *refs = refs
    pa_ref, pb_ref, gq_ref, ds_scr, w_scr = refs
    combos, rows, _ = q_ref.shape
    half = a_ref.shape[0] // 2
    pa_ref[...] = jnp.zeros_like(pa_ref)
    pb_ref[...] = jnp.zeros_like(pb_ref)

    def combo(c, carry):
        b, h = c // heads, c % heads
        wa, wb = tbl[b, ja], tbl[b, jb]
        own = block_of(kv_ref, b, h)
        ka, kb = key_of(a_ref, wa, h, own), key_of(b_ref, wb, h, own)
        v = rows_of(block_of(a_ref, wa, h, half), block_of(b_ref, wb, h, half))
        weights_and_grads(
            c, q_ref, o_ref, lse_ref, delta_ref, rows_of(ka, kb), v, ds_scr, w_scr
        )
        dk = dot(qt_ref[c], ds_scr[...])
        dv = dot(ot_ref[c], w_scr[...])
        for i, (ref, w) in enumerate(((pa_ref, wa), (pb_ref, wb))):
            src = slice(i * BLOCK, (i + 1) * BLOCK)
            ref[at(h, DH), at(slot(w), BLOCK)] += keep(w, dk[:, src])
            ref[at(heads + h, DH), at(slot(w), BLOCK)] += keep(w, dv[:, src])
        used = rows_of(keep(wa, ka), keep(wb, kb))
        for part in tiles(rows, BACK_TILE):
            grad = dot(ds_scr[part, :], used)
            gq_ref[c, part, :] = gq_in[c, part, :] + grad if has_sum else grad
        return carry

    lax.fori_loop(0, combos, combo, 0, unroll=BACK_UNROLL)


def back(tbl, slabs, kv, stats, a, b, gq, ja, jb, heads):
    combos, rows, _ = slabs[0].shape
    own_rows = a.shape[0] // 2
    extra = () if gq is None else (gq,)
    return call(
        functools.partial(back_kernel, heads, ja, jb, gq is not None),
        [SMEM] + [VMEM] * (9 + len(extra)),
        [f32((2 * heads * DH, own_rows))] * 2 + [f32((combos, rows, DH))],
        20 * combos * rows * BLOCK * DH,
        (tbl, *slabs, kv, *stats, a, b, *extra),
        [pltpu.VMEM((rows, 2 * BLOCK), jnp.bfloat16)] * 2,
    )


def own_kernel(
    heads, opposite, tbl, q_ref, o_ref, qt_ref, ot_ref, kv_ref, lse_ref, delta_ref, k4_ref,
    ds4_ref, att_ref, gq_in, att_out, gq_out, part_ref, ds_scr, w_scr, gq_scr, sems,
):
    combos, rows, _ = q_ref.shape
    group = rows // BLOCK
    half = kv_ref.shape[0] // 2

    def sends(ref, out, c, sem):
        b, h = c // heads, c % heads
        return [
            pltpu.make_async_copy(
                ref.at[c, pl.ds(g * BLOCK, BLOCK)],
                out.at[at(b, BLOCK), at(h * group + g, DH)],
                sem,
            )
            for g in range(group)
        ]

    def combo(c, carry):
        b, h = c // heads, c % heads
        for send in sends(att_ref, att_out, c, sems.at[0, c]):
            send.start()
        k, v = block_of(kv_ref, b, h), block_of(kv_ref, b, h, half)
        weights_and_grads(c, q_ref, o_ref, lse_ref, delta_ref, k, v, ds_scr, w_scr)
        part_ref[at(h, DH), at(b, BLOCK)] = dot(qt_ref[c], ds_scr[...])
        part_ref[at(heads + h, DH), at(b, BLOCK)] = dot(ot_ref[c], w_scr[...])
        w4 = tbl[b, opposite]
        used = rows_of(k, keep(w4, block_of(k4_ref, w4, h)))
        for part in tiles(rows, BACK_TILE):
            ds = jnp.concatenate([ds_scr[part, :], ds4_ref[c, part, :]], axis=1)
            grad = (gq_in[c, part, :] + dot(ds, used)) * SCALE
            gq_scr[c, part, :] = grad.astype(jnp.bfloat16)
        for send in sends(gq_scr, gq_out, c, sems.at[1, c]):
            send.start()
        return carry

    lax.fori_loop(0, combos, combo, 0)
    for c in range(combos):
        pltpu.make_async_copy(att_ref.at[c], att_ref.at[c], sems.at[0, c]).wait()
        pltpu.make_async_copy(gq_scr.at[c], gq_scr.at[c], sems.at[1, c]).wait()


def own(tbl, slabs, kv, stats, k4, ds4, att, gq, opposite, heads, q_shape):
    combos, rows, _ = slabs[0].shape
    return call(
        functools.partial(own_kernel, heads, opposite),
        [SMEM] + [VMEM] * 11,
        [bf16(q_shape), bf16(q_shape), f32((2 * heads * DH, kv.shape[0] // 2))],
        12 * combos * rows * BLOCK * DH,
        (tbl, *slabs, kv, *stats, k4, ds4, att, gq),
        [pltpu.VMEM((rows, BLOCK), jnp.bfloat16)] * 2
        + [pltpu.VMEM((combos, rows, DH), jnp.bfloat16), pltpu.SemaphoreType.DMA((2, combos))],
        [HBM, HBM, VMEM],
    )


def finish_kernel(own_ref, a_ref, b_ref, gk_ref, gv_ref):
    total = own_ref[...] + (a_ref[...].astype(jnp.float32) + b_ref[...].astype(jnp.float32))
    half = total.shape[0] // 2
    gk_ref[...] = (total[:half, :] * SCALE).T.astype(jnp.bfloat16)
    gv_ref[...] = total[half:, :].T.astype(jnp.bfloat16)


def local(queries, keys, values, grad_out, key_blocks, key_count):
    n = lax.axis_size("ctx")
    me = lax.axis_index("ctx")
    row_count, width = keys.shape
    blk_dev = row_count // BLOCK
    heads = width // DH
    group = QH // KVH
    combos = blk_dev * heads
    opposite = n // 2
    steps = opposite - 1

    order = list(range(0, n, 2)) + list(range(n - 1, 0, -2))
    up = [(order[i], order[(i + 1) % n]) for i in range(n)]
    down = [(b, a) for a, b in up]

    def place(index):
        return jnp.where(index % 2 == 0, index // 2, n - 1 - index // 2)

    def hop(x, perm):
        return lax.ppermute(x, "ctx", perm)

    kv = call(
        pack_kernel, [HBM] * 2, [bf16((2 * row_count, width))], 1e6, (keys, values),
        [pltpu.SemaphoreType.DMA((2,))],
    )[0]

    blocks = lax.dynamic_slice_in_dim(key_blocks, me * blk_dev, blk_dev, 0)
    counts = lax.dynamic_slice_in_dim(key_count, me * blk_dev, blk_dev, 0)
    live = jnp.arange(blocks.shape[1])[None, :] < counts[:, None]
    offset = (place(blocks // blk_dev) - place(me) + n) % n
    hit = live[:, :, None] & (offset[:, :, None] == jnp.arange(n)[None, None, :])
    tbl = jnp.sum(jnp.where(hit, (blocks % blk_dev)[:, :, None] + 1, 0), axis=1) - 1

    q, o, qt, ot, *state = first(queries, grad_out, kv, combos, heads, group)
    slabs = (q, o, qt, ot)
    behind, ahead = [kv], [kv]
    for s in range(1, steps + 1):
        behind.append(hop(behind[-1], up))
        ahead.append(hop(ahead[-1], down))
        state = near(tbl, q, kv, ahead[s], behind[s], state, s, n - s, heads)
    k4 = hop(behind[-1][:row_count], up)
    v4 = hop(ahead[-1][row_count:], down)

    att, lse, delta, ds4, pk, pv = turn(tbl, slabs, kv, k4, v4, state, opposite, heads)
    stats = (lse, delta)

    up_in = hop(pk, up)
    down_in = hop(pv, down)
    half = heads * DH
    gq = None
    for s in range(steps, 0, -1):
        part_a, part_b, gq = back(tbl, slabs, kv, stats, ahead[s], behind[s], gq, s, n - s, heads)
        if s == steps:
            up_out = jnp.concatenate([part_a[:half] + up_in.astype(jnp.float32), part_a[half:]])
            down_out = jnp.concatenate([part_b[:half], part_b[half:] + down_in.astype(jnp.float32)])
        else:
            up_out = part_a + up_in.astype(jnp.float32)
            down_out = part_b + down_in.astype(jnp.float32)
        up_in = hop(up_out.astype(jnp.bfloat16), up)
        down_in = hop(down_out.astype(jnp.bfloat16), down)
    attended, grad_q, own_part = own(
        tbl, slabs, kv, stats, k4, ds4, att, gq, opposite, heads, queries.shape
    )
    grad_k, grad_v = call(
        finish_kernel, [VMEM] * 3, [bf16(keys.shape)] * 2, 1e7,
        (own_part, up_in, down_in),
    )
    return attended, grad_q, grad_k, grad_v


def solution(mesh):
    spec = P("ctx", "head")
    return jax.shard_map(
        local,
        mesh=mesh,
        in_specs=(spec, spec, spec, spec, P(), P()),
        out_specs=(spec,) * 4,
        check_vma=False,
    )
```

```python
import functools
import math

import jax
import jax.numpy as jnp
from jax import lax
from jax.experimental import pallas as pl
from jax.experimental.pallas import tpu as pltpu
from jax.sharding import PartitionSpec as P


QH = 64
KVH = 8
DH = 128
BLOCK = 128
GROUP = QH // KVH
ROWS = GROUP * BLOCK
SUB = 8

SCALE = 1.0 / math.sqrt(DH)
EXP2_SCALE = SCALE * math.log2(math.e)
VMEM_BYTES = 24 * 1024 * 1024
FIRST_PART = 1024
NEAR_PART = 1024
TURN_PART = 1024
BACK_PART = 1024

NT = (((1,), (1,)), ((), ()))
VMEM = pl.BlockSpec(memory_space=pltpu.VMEM)
SMEM = pl.BlockSpec(memory_space=pltpu.SMEM)
HBM = pl.BlockSpec(memory_space=pltpu.HBM)


def dot(a, b):
    return jnp.dot(a, b, preferred_element_type=jnp.float32)


def dot_t(a, b):
    return lax.dot_general(a, b, NT, preferred_element_type=jnp.float32)


def bf16(shape):
    return jax.ShapeDtypeStruct(shape, jnp.bfloat16)


def f32(shape):
    return jax.ShapeDtypeStruct(shape, jnp.float32)


def call(kernel, in_specs, out_shape, flops, args, scratch=(), out_specs=None, size=1 << 20):
    return pl.pallas_call(
        kernel,
        in_specs=in_specs,
        out_specs=out_specs or [VMEM] * len(out_shape),
        out_shape=out_shape,
        scratch_shapes=list(scratch),
        compiler_params=pltpu.CompilerParams(vmem_limit_bytes=VMEM_BYTES),
        cost_estimate=pl.CostEstimate(
            flops=int(flops), bytes_accessed=size, transcendentals=0
        ),
    )(*args)


def at(index, size):
    if isinstance(index, int):
        return pl.ds(index * size, size)
    return pl.ds(pl.multiple_of(index * size, size), size)


def slot(w):
    return w if isinstance(w, int) else jnp.maximum(w, 0)


def block_of(ref, w, h):
    return ref[at(slot(w), BLOCK), at(h, DH)]


def key_of(ref, w, h, own):
    return jnp.where(w >= 0, block_of(ref, w, h), own)


def keep(w, x):
    return jnp.where(w >= 0, x, jnp.zeros_like(x))


def value_t(v, w):
    return keep(w, jnp.concatenate([v.T, jnp.ones((2 * SUB, BLOCK), v.dtype)], axis=0))


def queries_of(ref, b, h, part):
    members = range(part.start // BLOCK, part.stop // BLOCK)
    return jnp.concatenate(
        [ref[at(b, BLOCK), at(h * GROUP + g, DH)] for g in members], axis=0
    )


def split(x):
    return x.reshape(x.shape[0] // SUB, SUB, x.shape[1])


def join(x):
    return x.reshape(x.shape[0] * SUB, x.shape[2])


def all_equal(x):
    return jnp.broadcast_to(jnp.sum(x, axis=0, keepdims=True), x.shape)


def largest(x):
    top = jnp.max(x, axis=0)
    return jnp.broadcast_to(jnp.max(top, axis=0, keepdims=True), top.shape)


def parts(size):
    return [slice(t, t + size) for t in range(0, ROWS, size)]


def staggered(combos, size, phases):
    waiting = [phases(c, part) for c in range(combos) for part in parts(size)]
    active = []
    while waiting or active:
        if waiting:
            active.append(waiting.pop(0))
        active = [g for g in active if next(g, "end") != "end"]


def eye(size):
    row = lax.broadcasted_iota(jnp.int32, (size, size), 0)
    return jnp.where(row == lax.broadcasted_iota(jnp.int32, (size, size), 1), 1.0, 0.0).astype(
        jnp.bfloat16
    )


def table_kernel(slots_ref, counts_ref, tbl):
    blk_dev, n = tbl.shape
    me = lax.axis_index("ctx")

    def place(index):
        half = lax.shift_right_logical(index, 1)
        return jnp.where(lax.bitwise_and(index, 1) == 0, half, n - 1 - half)

    for b in range(blk_dev):
        for j in range(n):
            tbl[b, j] = -1
        row = me * blk_dev + b
        for s in range(slots_ref.shape[0]):
            block = slots_ref[s, row]
            owner = lax.div(block, blk_dev)
            offset = lax.rem(place(owner) - place(me) + n, n)

            @pl.when(s < counts_ref[row])
            def _():
                tbl[b, offset] = block - owner * blk_dev


def table(blocks, counts, blk_dev, n):
    return call(
        table_kernel, [SMEM] * 2, [jax.ShapeDtypeStruct((blk_dev, n), jnp.int32)], 1e10,
        (blocks.T, counts), out_specs=[SMEM], size=1 << 26,
    )[0]


def first_kernel(heads, q_ref, o_ref, k_ref, v_ref, ot_ref, acc_ref, m_ref):
    unit = eye(DH)

    def phases(c, part):
        b, h = c // heads, c % heads
        k = block_of(k_ref, b, h)
        x = dot_t(k, queries_of(q_ref, b, h, part))
        turned = dot_t(unit, queries_of(o_ref, b, h, part))
        yield
        v = value_t(block_of(v_ref, b, h), 0)
        x = split(x * EXP2_SCALE)
        m = largest(x)
        m_ref[c, :, part] = m
        p = join(jnp.exp2(x - m)).astype(jnp.bfloat16)
        ot_ref[c, :, part] = turned.astype(jnp.bfloat16)
        yield
        acc_ref[c, :, part] = dot(v, p)[: DH + SUB]

    staggered(m_ref.shape[0], FIRST_PART, phases)


def first(q, o, k, v, combos, heads):
    return call(
        functools.partial(first_kernel, heads),
        [VMEM] * 4,
        [bf16((combos, DH, ROWS)), f32((combos, DH + SUB, ROWS)), f32((combos, SUB, ROWS))],
        6 * combos * ROWS * BLOCK * DH,
        (q, o, k, v),
    )


def near_kernel(
    heads, ja, jb, tbl, q_ref, own_ref, ka_ref, va_ref, kb_ref, vb_ref, acc_in, m_in, acc_ref, m_ref
):
    def phases(c, part):
        b, h = c // heads, c % heads
        wa, wb = tbl[b, ja], tbl[b, jb]
        own = block_of(own_ref, b, h)
        k = jnp.concatenate([key_of(ka_ref, wa, h, own), key_of(kb_ref, wb, h, own)], axis=0)
        x = dot_t(k, queries_of(q_ref, b, h, part))
        yield
        v = jnp.concatenate(
            [value_t(block_of(va_ref, wa, h), wa), value_t(block_of(vb_ref, wb, h), wb)], axis=1
        )
        x = split(x * EXP2_SCALE)
        old = m_in[c, :, part]
        m = jnp.maximum(old, largest(x))
        p = join(jnp.exp2(x - m)).astype(jnp.bfloat16)
        m_ref[c, :, part] = m
        yield
        acc = join(split(acc_in[c, :, part]) * jnp.exp2(old - m))
        acc_ref[c, :, part] = acc + dot(v, p)[: DH + SUB]

    staggered(m_ref.shape[0], NEAR_PART, phases)


def near(tbl, q, k_own, ahead, behind, state, ja, jb, heads):
    combos = state[1].shape[0]
    return call(
        functools.partial(near_kernel, heads, ja, jb),
        [SMEM] + [VMEM] * 8,
        [f32(a.shape) for a in state],
        8 * combos * ROWS * BLOCK * DH,
        (tbl, q, k_own, *ahead, *behind, *state),
    )


def turn_kernel(
    heads, opposite, tbl, q_ref, o_ref, ot_ref, own_ref, k_ref, v_ref, acc_in, m_in,
    att_ref, lse_ref, delta_ref, ds_ref, pk_ref, pv_ref, pk_scr, pv_scr,
):
    pk_scr[...] = jnp.zeros_like(pk_scr)
    pv_scr[...] = jnp.zeros_like(pv_scr)

    def phases(c, part):
        b, h = c // heads, c % heads
        w = tbl[b, opposite]
        k = key_of(k_ref, w, h, block_of(own_ref, b, h))
        v = block_of(v_ref, w, h)
        q, o = queries_of(q_ref, b, h, part), queries_of(o_ref, b, h, part)
        x = dot_t(k, q)
        yield
        grad_p = split(dot_t(v, o))
        v_t = value_t(v, w)
        x = split(x * EXP2_SCALE)
        old = m_in[c, :, part]
        m = jnp.maximum(old, largest(x))
        p = jnp.exp2(x - m)
        acc = dot(v_t, join(p).astype(jnp.bfloat16))[: DH + SUB]
        yield
        acc = split(acc_in[c, :, part]) * jnp.exp2(old - m) + split(acc)
        total = acc[DH // SUB]
        inverse = 1.0 / total
        att = join(acc[: DH // SUB] * inverse).astype(jnp.bfloat16)
        att_ref[c, :, part] = att
        terms = att.astype(jnp.float32) * ot_ref[c, :, part].astype(jnp.float32)
        delta = all_equal(jnp.sum(split(terms), axis=0))
        p = p * inverse
        weights = join(p).astype(jnp.bfloat16)
        ds = join(p * (grad_p - delta)).astype(jnp.bfloat16)
        ds_ref[c, :, part] = ds
        lse_ref[c, :, part] = m + jnp.log2(total)
        delta_ref[c, :, part] = delta
        yield
        pk_scr[at(slot(w), BLOCK), h * DH : (h + 1) * DH] += keep(w, dot(ds, q))
        pv_scr[at(slot(w), BLOCK), h * DH : (h + 1) * DH] += keep(w, dot(weights, o))

    staggered(m_in.shape[0], TURN_PART, phases)
    pk_ref[...] = pk_scr[...].astype(jnp.bfloat16)
    pv_ref[...] = pv_scr[...].astype(jnp.bfloat16)


def turn(tbl, q, o, ot, k_own, k4, v4, state, opposite, heads):
    combos = ot.shape[0]
    return call(
        functools.partial(turn_kernel, heads, opposite),
        [SMEM] + [VMEM] * 8,
        [bf16(ot.shape)]
        + [f32((combos, SUB, ROWS))] * 2
        + [bf16((combos, BLOCK, ROWS))]
        + [bf16(k4.shape)] * 2,
        10 * combos * ROWS * BLOCK * DH,
        (tbl, q, o, ot, k_own, k4, v4, *state),
        [pltpu.VMEM(k4.shape, jnp.float32)] * 2,
    )


def weights_and_grads(c, part, x, grad_p, lse_ref, delta_ref):
    p = jnp.exp2(split(x * EXP2_SCALE) - lse_ref[c, :, part])
    ds = p * (split(grad_p) - delta_ref[c, :, part])
    return join(p).astype(jnp.bfloat16), join(ds).astype(jnp.bfloat16)


def back_kernel(
    heads, ja, jb, has_sum, tbl, q_ref, o_ref, own_ref, lse_ref, delta_ref, ka_ref, va_ref,
    kb_ref, vb_ref, *refs,
):
    if has_sum:
        gq_in, *refs = refs
    pka_ref, pva_ref, pkb_ref, pvb_ref, gq_ref = refs
    for ref in (pka_ref, pva_ref, pkb_ref, pvb_ref):
        ref[...] = jnp.zeros_like(ref)

    def phases(c, part):
        b, h = c // heads, c % heads
        wa, wb = tbl[b, ja], tbl[b, jb]
        own = block_of(own_ref, b, h)
        ka, kb = key_of(ka_ref, wa, h, own), key_of(kb_ref, wb, h, own)
        v = jnp.concatenate([block_of(va_ref, wa, h), block_of(vb_ref, wb, h)], axis=0)
        q, o = queries_of(q_ref, b, h, part), queries_of(o_ref, b, h, part)
        x = dot_t(jnp.concatenate([ka, kb], axis=0), q)
        grad_p = dot_t(v, o)
        yield
        weights, ds = weights_and_grads(c, part, x, grad_p, lse_ref, delta_ref)
        yield
        dk, dv = dot(ds, q), dot(weights, o)
        lanes = slice(h * DH, (h + 1) * DH)
        for i, (rk, rv, w) in enumerate(((pka_ref, pva_ref, wa), (pkb_ref, pvb_ref, wb))):
            src = slice(i * BLOCK, (i + 1) * BLOCK)
            rk[at(slot(w), BLOCK), lanes] += keep(w, dk[src])
            rv[at(slot(w), BLOCK), lanes] += keep(w, dv[src])
        grad = dot(jnp.concatenate([keep(wa, ka).T, keep(wb, kb).T], axis=1), ds)
        gq_ref[c, :, part] = gq_in[c, :, part] + grad if has_sum else grad

    staggered(gq_ref.shape[0], BACK_PART, phases)


def back(tbl, q, o, k_own, stats, ahead, behind, gq, ja, jb, heads):
    combos = stats[0].shape[0]
    extra = () if gq is None else (gq,)
    return call(
        functools.partial(back_kernel, heads, ja, jb, gq is not None),
        [SMEM] + [VMEM] * (9 + len(extra)),
        [f32(k_own.shape)] * 4 + [f32((combos, DH, ROWS))],
        20 * combos * ROWS * BLOCK * DH,
        (tbl, q, o, k_own, *stats, *ahead, *behind, *extra),
    )


def own_kernel(
    heads, opposite, tbl, q_ref, o_ref, k_ref, v_ref, lse_ref, delta_ref, k4_ref, ds4_ref,
    att_ref, gq_in, att_out, gq_out, pk_ref, pv_ref, att_scr, gq_scr, sems,
):
    combos = gq_in.shape[0]
    unit = eye(2 * BLOCK)

    def send(ref, out, c, kind):
        b, h = c // heads, c % heads
        place = (at(b, BLOCK), at(h, GROUP * DH))
        return pltpu.make_async_copy(ref.at[place], out.at[place], sems.at[kind, c])

    def put(ref, b, h, x):
        for i in range(GROUP // 2):
            y = dot_t(unit, x[:, i * 2 * BLOCK : (i + 1) * 2 * BLOCK]).astype(jnp.bfloat16)
            for j in range(2):
                place = (at(b, BLOCK), at(h * GROUP + 2 * i + j, DH))
                ref[place] = y[j * BLOCK : (j + 1) * BLOCK]

    def phases(c, part):
        b, h = c // heads, c % heads
        q, o = queries_of(q_ref, b, h, part), queries_of(o_ref, b, h, part)
        k = block_of(k_ref, b, h)
        x, grad_p = dot_t(k, q), dot_t(block_of(v_ref, b, h), o)
        yield
        weights, ds = weights_and_grads(c, part, x, grad_p, lse_ref, delta_ref)
        put(att_scr, b, h, att_ref[c])
        send(att_scr, att_out, c, 0).start()
        yield
        place = (at(b, BLOCK), at(h, DH))
        pk_ref[place] = dot(ds, q)
        pv_ref[place] = dot(weights, o)
        w4 = tbl[b, opposite]
        used = jnp.concatenate([k.T, keep(w4, block_of(k4_ref, w4, h)).T], axis=1)
        grad = (gq_in[c] + dot(used, jnp.concatenate([ds, ds4_ref[c]], axis=0))) * SCALE
        yield
        put(gq_scr, b, h, grad.astype(jnp.bfloat16))
        send(gq_scr, gq_out, c, 1).start()

    staggered(combos, ROWS, phases)
    for c in range(combos):
        send(att_scr, att_out, c, 0).wait()
        send(gq_scr, gq_out, c, 1).wait()


def own(tbl, q, o, k, v, stats, k4, ds4, att, gq, opposite, heads):
    combos = gq.shape[0]
    return call(
        functools.partial(own_kernel, heads, opposite),
        [SMEM] + [VMEM] * 10,
        [bf16(q.shape), bf16(q.shape), f32(k.shape), f32(k.shape)],
        12 * combos * ROWS * BLOCK * DH,
        (tbl, q, o, k, v, *stats, k4, ds4, att, gq),
        [pltpu.VMEM(q.shape, jnp.bfloat16)] * 2
        + [pltpu.SemaphoreType.DMA((2, combos))],
        [HBM, HBM, VMEM, VMEM],
    )


def finish_kernel(pk_ref, ka_ref, kb_ref, pv_ref, va_ref, vb_ref, gk_ref, gv_ref):
    def total(own, a, b):
        return own[...] + (a[...].astype(jnp.float32) + b[...].astype(jnp.float32))

    gk_ref[...] = (total(pk_ref, ka_ref, kb_ref) * SCALE).astype(jnp.bfloat16)
    gv_ref[...] = total(pv_ref, va_ref, vb_ref).astype(jnp.bfloat16)


def finish(*args):
    return call(finish_kernel, [VMEM] * 6, [bf16(args[0].shape)] * 2, 1e7, args)


def local(queries, keys, values, grad_out, key_blocks, key_count):
    n = lax.axis_size("ctx")
    row_count, width = keys.shape
    blk_dev = row_count // BLOCK
    heads = width // DH
    combos = blk_dev * heads
    opposite = n // 2
    steps = opposite - 1

    order = list(range(0, n, 2)) + list(range(n - 1, 0, -2))
    up = [(order[i], order[(i + 1) % n]) for i in range(n)]
    ways = {"up": up, "down": [(b, a) for a, b in up]}

    def hop(x, way):
        return lax.ppermute(x, "ctx", ways[way])

    behind, ahead = [(keys, values)], [(keys, values)]
    tbl = table(key_blocks, key_count, blk_dev, n)
    ot, *state = first(queries, grad_out, keys, values, combos, heads)
    for s in range(1, steps + 1):
        k_up = hop(behind[-1][0], "up")
        k_down = hop(ahead[-1][0], "down")
        v_up = hop(behind[-1][1], "up")
        v_down = hop(ahead[-1][1], "down")
        behind.append((k_up, v_up))
        ahead.append((k_down, v_down))
        state = near(
            tbl, queries, keys, ahead[s], behind[s], state, s, n - s, heads
        )
    k4 = hop(behind[-1][0], "up")
    v4 = hop(ahead[-1][1], "down")

    att, lse, delta, ds4, pk, pv = turn(
        tbl, queries, grad_out, ot, keys, k4, v4, state, opposite, heads
    )
    stats = (lse, delta)

    def plus(part, x):
        return part if x is None else part + x.astype(jnp.float32)

    k_up, k_down = hop(pk, "up"), None
    v_up, v_down = None, hop(pv, "down")
    gq = None
    for s in range(steps, 0, -1):
        pka, pva, pkb, pvb, gq = back(
            tbl, queries, grad_out, keys, stats, ahead[s], behind[s], gq, s, n - s, heads
        )
        k_up = hop(plus(pka, k_up).astype(jnp.bfloat16), "up")
        k_down = hop(plus(pkb, k_down).astype(jnp.bfloat16), "down")
        v_up = hop(plus(pva, v_up).astype(jnp.bfloat16), "up")
        v_down = hop(plus(pvb, v_down).astype(jnp.bfloat16), "down")
    attended, grad_q, pk, pv = own(
        tbl, queries, grad_out, keys, values, stats, k4, ds4, att, gq, opposite, heads
    )
    grad_k, grad_v = finish(pk, k_up, k_down, pv, v_up, v_down)
    return attended, grad_q, grad_k, grad_v


def solution(mesh):
    spec = P("ctx", "head")
    return jax.shard_map(
        local,
        mesh=mesh,
        in_specs=(spec, spec, spec, spec, P(), P()),
        out_specs=(spec,) * 4,
        check_vma=False,
    )
```

```python
import functools
import math

import jax
import jax.numpy as jnp
from jax import lax
from jax.experimental import pallas as pl
from jax.experimental.pallas import tpu as pltpu
from jax.sharding import PartitionSpec as P


QH = 64
KVH = 8
DH = 128
BLOCK = 128
GROUP = QH // KVH
ROWS = GROUP * BLOCK
SUB = 8

SCALE = 1.0 / math.sqrt(DH)
EXP2_SCALE = SCALE * math.log2(math.e)
VMEM_BYTES = 24 * 1024 * 1024
FIRST_PART = 1024
NEAR_PART = 1024
TURN_PART = 1024
BACK_PART = 1024

NT = (((1,), (1,)), ((), ()))
VMEM = pl.BlockSpec(memory_space=pltpu.VMEM)
SMEM = pl.BlockSpec(memory_space=pltpu.SMEM)
HBM = pl.BlockSpec(memory_space=pltpu.HBM)


def dot(a, b):
    return jnp.dot(a, b, preferred_element_type=jnp.float32)


def dot_t(a, b):
    return lax.dot_general(a, b, NT, preferred_element_type=jnp.float32)


def bf16(shape):
    return jax.ShapeDtypeStruct(shape, jnp.bfloat16)


def f32(shape):
    return jax.ShapeDtypeStruct(shape, jnp.float32)


def call(kernel, in_specs, out_shape, flops, args, scratch=(), out_specs=None, size=1 << 20):
    return pl.pallas_call(
        kernel,
        in_specs=in_specs,
        out_specs=out_specs or [VMEM] * len(out_shape),
        out_shape=out_shape,
        scratch_shapes=list(scratch),
        compiler_params=pltpu.CompilerParams(vmem_limit_bytes=VMEM_BYTES),
        cost_estimate=pl.CostEstimate(
            flops=int(flops), bytes_accessed=size, transcendentals=0
        ),
    )(*args)


def at(index, size):
    if isinstance(index, int):
        return pl.ds(index * size, size)
    return pl.ds(pl.multiple_of(index * size, size), size)


def block(ref, i, h):
    return ref[i * BLOCK : (i + 1) * BLOCK, h * DH : (h + 1) * DH]


def tall(tile):
    return jnp.concatenate([tile] * (BLOCK // tile.shape[0]), axis=0)


class Pick:
    def __init__(self, table_ref, j, b):
        self.count = table_ref.shape[2] - 1
        self.tiles = [table_ref[j, b, i] for i in range(self.count + 1)]

    def listed(self, ref, h):
        terms = [block(ref, i, h) * tall(self.tiles[i]) for i in range(self.count)]
        return functools.reduce(jnp.add, terms)

    def key(self, ref, h, own):
        return self.listed(ref, h) + own * tall(self.tiles[self.count])

    def value_t(self, v):
        return jnp.concatenate([v.T, functools.reduce(jnp.add, self.tiles[: self.count])], axis=0)

    def add(self, ref, h, x):
        for i in range(self.count):
            factor = tall(self.tiles[i].astype(jnp.float32))
            ref[i * BLOCK : (i + 1) * BLOCK, h * DH : (h + 1) * DH] += x * factor


def queries_of(ref, b, h, part):
    members = range(part.start // BLOCK, part.stop // BLOCK)
    return jnp.concatenate(
        [ref[at(b, BLOCK), at(h * GROUP + g, DH)] for g in members], axis=0
    )


def split(x):
    return x.reshape(x.shape[0] // SUB, SUB, x.shape[1])


def join(x):
    return x.reshape(x.shape[0] * SUB, x.shape[2])


def all_equal(x):
    return jnp.broadcast_to(jnp.sum(x, axis=0, keepdims=True), x.shape)


def largest(x):
    top = jnp.max(x, axis=0)
    return jnp.broadcast_to(jnp.max(top, axis=0, keepdims=True), top.shape)


def parts(size):
    return [slice(t, t + size) for t in range(0, ROWS, size)]


def staggered(combos, size, phases):
    waiting = [phases(c, part) for c in range(combos) for part in parts(size)]
    active = []
    while waiting or active:
        if waiting:
            active.append(waiting.pop(0))
        active = [g for g in active if next(g, "end") != "end"]


def eye(size):
    row = lax.broadcasted_iota(jnp.int32, (size, size), 0)
    return jnp.where(row == lax.broadcasted_iota(jnp.int32, (size, size), 1), 1.0, 0.0).astype(
        jnp.bfloat16
    )


def table_kernel(slots_ref, counts_ref, out_ref, tbl):
    blk_dev, n = tbl.shape
    me = lax.axis_index("ctx")

    def place(index):
        half = lax.shift_right_logical(index, 1)
        return jnp.where(lax.bitwise_and(index, 1) == 0, half, n - 1 - half)

    for b in range(blk_dev):
        for j in range(n):
            tbl[b, j] = blk_dev
        row = me * blk_dev + b
        for s in range(slots_ref.shape[0]):
            listed = slots_ref[s, row]
            owner = lax.div(listed, blk_dev)
            offset = lax.rem(place(owner) - place(me) + n, n)

            @pl.when(s < counts_ref[row])
            def _():
                tbl[b, offset] = listed - owner * blk_dev

        for j in range(n):
            for i in range(blk_dev + 1):
                value = jnp.where(tbl[b, j] == i, 1.0, 0.0)
                out_ref[j, b, i] = jnp.full((2 * SUB, DH), value, jnp.float32).astype(jnp.bfloat16)


def table(blocks, counts, blk_dev, n):
    return call(
        table_kernel, [SMEM] * 2, [bf16((n, blk_dev, blk_dev + 1, 2 * SUB, DH))], 1e10,
        (blocks.T, counts), [pltpu.SMEM((blk_dev, n), jnp.int32)], size=1 << 26,
    )[0]


def first_kernel(heads, q_ref, o_ref, k_ref, v_ref, ot_ref, acc_ref, m_ref):
    unit = eye(DH)

    def phases(c, part):
        b, h = c // heads, c % heads
        x = dot_t(block(k_ref, b, h), queries_of(q_ref, b, h, part))
        turned = dot_t(unit, queries_of(o_ref, b, h, part))
        yield
        v = block(v_ref, b, h).T
        v = jnp.concatenate([v, jnp.ones((2 * SUB, BLOCK), v.dtype)], axis=0)
        x = split(x * EXP2_SCALE)
        m = largest(x)
        m_ref[c, :, part] = m
        p = join(jnp.exp2(x - m)).astype(jnp.bfloat16)
        ot_ref[c, :, part] = turned.astype(jnp.bfloat16)
        yield
        acc_ref[c, :, part] = dot(v, p)[: DH + SUB]

    staggered(m_ref.shape[0], FIRST_PART, phases)


def first(q, o, k, v, combos, heads):
    return call(
        functools.partial(first_kernel, heads),
        [VMEM] * 4,
        [bf16((combos, DH, ROWS)), f32((combos, DH + SUB, ROWS)), f32((combos, SUB, ROWS))],
        6 * combos * ROWS * BLOCK * DH,
        (q, o, k, v),
    )


def near_kernel(
    heads, ja, jb, tbl, q_ref, own_ref, ka_ref, va_ref, kb_ref, vb_ref, acc_in, m_in, acc_ref, m_ref
):
    def phases(c, part):
        b, h = c // heads, c % heads
        pa, pb = Pick(tbl, ja, b), Pick(tbl, jb, b)
        own = block(own_ref, b, h)
        k = jnp.concatenate([pa.key(ka_ref, h, own), pb.key(kb_ref, h, own)], axis=0)
        x = dot_t(k, queries_of(q_ref, b, h, part))
        yield
        v = jnp.concatenate(
            [pa.value_t(pa.listed(va_ref, h)), pb.value_t(pb.listed(vb_ref, h))], axis=1
        )
        x = split(x * EXP2_SCALE)
        old = m_in[c, :, part]
        m = jnp.maximum(old, largest(x))
        p = join(jnp.exp2(x - m)).astype(jnp.bfloat16)
        m_ref[c, :, part] = m
        yield
        acc = join(split(acc_in[c, :, part]) * jnp.exp2(old - m))
        acc_ref[c, :, part] = acc + dot(v, p)[: DH + SUB]

    staggered(m_ref.shape[0], NEAR_PART, phases)


def near(tbl, q, k_own, ahead, behind, state, ja, jb, heads):
    combos = state[1].shape[0]
    return call(
        functools.partial(near_kernel, heads, ja, jb),
        [VMEM] * 9,
        [f32(a.shape) for a in state],
        8 * combos * ROWS * BLOCK * DH,
        (tbl, q, k_own, *ahead, *behind, *state),
    )


def turn_kernel(
    heads, opposite, tbl, q_ref, o_ref, ot_ref, own_ref, k_ref, v_ref, acc_in, m_in,
    att_ref, lse_ref, delta_ref, ds_ref, pk_ref, pv_ref, pk_scr, pv_scr,
):
    pk_scr[...] = jnp.zeros_like(pk_scr)
    pv_scr[...] = jnp.zeros_like(pv_scr)

    def phases(c, part):
        b, h = c // heads, c % heads
        pick = Pick(tbl, opposite, b)
        k = pick.key(k_ref, h, block(own_ref, b, h))
        v = pick.listed(v_ref, h)
        q, o = queries_of(q_ref, b, h, part), queries_of(o_ref, b, h, part)
        x = dot_t(k, q)
        yield
        grad_p = split(dot_t(v, o))
        v_t = pick.value_t(v)
        x = split(x * EXP2_SCALE)
        old = m_in[c, :, part]
        m = jnp.maximum(old, largest(x))
        p = jnp.exp2(x - m)
        acc = dot(v_t, join(p).astype(jnp.bfloat16))[: DH + SUB]
        yield
        acc = split(acc_in[c, :, part]) * jnp.exp2(old - m) + split(acc)
        total = acc[DH // SUB]
        inverse = 1.0 / total
        att = join(acc[: DH // SUB] * inverse).astype(jnp.bfloat16)
        att_ref[c, :, part] = att
        terms = att.astype(jnp.float32) * ot_ref[c, :, part].astype(jnp.float32)
        delta = all_equal(jnp.sum(split(terms), axis=0))
        p = p * inverse
        weights = join(p).astype(jnp.bfloat16)
        ds = join(p * (grad_p - delta)).astype(jnp.bfloat16)
        ds_ref[c, :, part] = ds
        lse_ref[c, :, part] = m + jnp.log2(total)
        delta_ref[c, :, part] = delta
        yield
        pick.add(pk_scr, h, dot(ds, q))
        pick.add(pv_scr, h, dot(weights, o))

    staggered(m_in.shape[0], TURN_PART, phases)
    pk_ref[...] = pk_scr[...].astype(jnp.bfloat16)
    pv_ref[...] = pv_scr[...].astype(jnp.bfloat16)


def turn(tbl, q, o, ot, k_own, k4, v4, state, opposite, heads):
    combos = ot.shape[0]
    return call(
        functools.partial(turn_kernel, heads, opposite),
        [VMEM] * 9,
        [bf16(ot.shape)]
        + [f32((combos, SUB, ROWS))] * 2
        + [bf16((combos, BLOCK, ROWS))]
        + [bf16(k4.shape)] * 2,
        10 * combos * ROWS * BLOCK * DH,
        (tbl, q, o, ot, k_own, k4, v4, *state),
        [pltpu.VMEM(k4.shape, jnp.float32)] * 2,
    )


def weights_and_grads(c, part, x, grad_p, lse_ref, delta_ref):
    p = jnp.exp2(split(x * EXP2_SCALE) - lse_ref[c, :, part])
    ds = p * (split(grad_p) - delta_ref[c, :, part])
    return join(p).astype(jnp.bfloat16), join(ds).astype(jnp.bfloat16)


def back_kernel(
    heads, ja, jb, has_sum, tbl, q_ref, o_ref, own_ref, lse_ref, delta_ref, ka_ref, va_ref,
    kb_ref, vb_ref, *refs,
):
    if has_sum:
        gq_in, *refs = refs
    pka_ref, pva_ref, pkb_ref, pvb_ref, gq_ref = refs
    for ref in (pka_ref, pva_ref, pkb_ref, pvb_ref):
        ref[...] = jnp.zeros_like(ref)

    def phases(c, part):
        b, h = c // heads, c % heads
        pa, pb = Pick(tbl, ja, b), Pick(tbl, jb, b)
        own = block(own_ref, b, h)
        k = jnp.concatenate([pa.key(ka_ref, h, own), pb.key(kb_ref, h, own)], axis=0)
        v = jnp.concatenate([pa.listed(va_ref, h), pb.listed(vb_ref, h)], axis=0)
        q, o = queries_of(q_ref, b, h, part), queries_of(o_ref, b, h, part)
        x = dot_t(k, q)
        grad_p = dot_t(v, o)
        yield
        weights, ds = weights_and_grads(c, part, x, grad_p, lse_ref, delta_ref)
        yield
        dk, dv = dot(ds, q), dot(weights, o)
        for i, (pick, rk, rv) in enumerate(((pa, pka_ref, pva_ref), (pb, pkb_ref, pvb_ref))):
            src = slice(i * BLOCK, (i + 1) * BLOCK)
            pick.add(rk, h, dk[src])
            pick.add(rv, h, dv[src])
        used = jnp.concatenate([pa.listed(ka_ref, h).T, pb.listed(kb_ref, h).T], axis=1)
        grad = dot(used, ds)
        gq_ref[c, :, part] = gq_in[c, :, part] + grad if has_sum else grad

    staggered(gq_ref.shape[0], BACK_PART, phases)


def back(tbl, q, o, k_own, stats, ahead, behind, gq, ja, jb, heads):
    combos = stats[0].shape[0]
    extra = () if gq is None else (gq,)
    return call(
        functools.partial(back_kernel, heads, ja, jb, gq is not None),
        [VMEM] * (10 + len(extra)),
        [f32(k_own.shape)] * 4 + [f32((combos, DH, ROWS))],
        20 * combos * ROWS * BLOCK * DH,
        (tbl, q, o, k_own, *stats, *ahead, *behind, *extra),
    )


def own_kernel(
    heads, opposite, tbl, q_ref, o_ref, k_ref, v_ref, lse_ref, delta_ref, k4_ref, ds4_ref,
    att_ref, gq_in, att_out, gq_out, pk_ref, pv_ref, att_scr, gq_scr, sems,
):
    combos = gq_in.shape[0]
    unit = eye(2 * BLOCK)

    def send(ref, out, c, kind):
        b, h = c // heads, c % heads
        place = (at(b, BLOCK), at(h, GROUP * DH))
        return pltpu.make_async_copy(ref.at[place], out.at[place], sems.at[kind, c])

    def put(ref, b, h, x):
        for i in range(GROUP // 2):
            y = dot_t(unit, x[:, i * 2 * BLOCK : (i + 1) * 2 * BLOCK]).astype(jnp.bfloat16)
            for j in range(2):
                place = (at(b, BLOCK), at(h * GROUP + 2 * i + j, DH))
                ref[place] = y[j * BLOCK : (j + 1) * BLOCK]

    def phases(c, part):
        b, h = c // heads, c % heads
        q, o = queries_of(q_ref, b, h, part), queries_of(o_ref, b, h, part)
        k = block(k_ref, b, h)
        x, grad_p = dot_t(k, q), dot_t(block(v_ref, b, h), o)
        yield
        weights, ds = weights_and_grads(c, part, x, grad_p, lse_ref, delta_ref)
        put(att_scr, b, h, att_ref[c])
        send(att_scr, att_out, c, 0).start()
        yield
        place = (at(b, BLOCK), at(h, DH))
        pk_ref[place] = dot(ds, q)
        pv_ref[place] = dot(weights, o)
        used = jnp.concatenate([k.T, Pick(tbl, opposite, b).listed(k4_ref, h).T], axis=1)
        grad = (gq_in[c] + dot(used, jnp.concatenate([ds, ds4_ref[c]], axis=0))) * SCALE
        yield
        put(gq_scr, b, h, grad.astype(jnp.bfloat16))
        send(gq_scr, gq_out, c, 1).start()

    staggered(combos, ROWS, phases)
    for c in range(combos):
        send(att_scr, att_out, c, 0).wait()
        send(gq_scr, gq_out, c, 1).wait()


def own(tbl, q, o, k, v, stats, k4, ds4, att, gq, opposite, heads):
    combos = gq.shape[0]
    return call(
        functools.partial(own_kernel, heads, opposite),
        [VMEM] * 11,
        [bf16(q.shape), bf16(q.shape), f32(k.shape), f32(k.shape)],
        12 * combos * ROWS * BLOCK * DH,
        (tbl, q, o, k, v, *stats, k4, ds4, att, gq),
        [pltpu.VMEM(q.shape, jnp.bfloat16)] * 2
        + [pltpu.SemaphoreType.DMA((2, combos))],
        [HBM, HBM, VMEM, VMEM],
    )


def finish_kernel(pk_ref, ka_ref, kb_ref, pv_ref, va_ref, vb_ref, gk_ref, gv_ref):
    def total(own, a, b):
        return own[...] + (a[...].astype(jnp.float32) + b[...].astype(jnp.float32))

    gk_ref[...] = (total(pk_ref, ka_ref, kb_ref) * SCALE).astype(jnp.bfloat16)
    gv_ref[...] = total(pv_ref, va_ref, vb_ref).astype(jnp.bfloat16)


def finish(*args):
    return call(finish_kernel, [VMEM] * 6, [bf16(args[0].shape)] * 2, 1e7, args)


def local(queries, keys, values, grad_out, key_blocks, key_count):
    n = lax.axis_size("ctx")
    row_count, width = keys.shape
    blk_dev = row_count // BLOCK
    heads = width // DH
    combos = blk_dev * heads
    opposite = n // 2
    steps = opposite - 1

    order = list(range(0, n, 2)) + list(range(n - 1, 0, -2))
    up = [(order[i], order[(i + 1) % n]) for i in range(n)]
    ways = {"up": up, "down": [(b, a) for a, b in up]}

    def hop(x, way):
        return lax.ppermute(x, "ctx", ways[way])

    behind, ahead = [(keys, values)], [(keys, values)]
    tbl = table(key_blocks, key_count, blk_dev, n)
    ot, *state = first(queries, grad_out, keys, values, combos, heads)
    for s in range(1, steps + 1):
        k_up = hop(behind[-1][0], "up")
        k_down = hop(ahead[-1][0], "down")
        v_up = hop(behind[-1][1], "up")
        v_down = hop(ahead[-1][1], "down")
        behind.append((k_up, v_up))
        ahead.append((k_down, v_down))
        state = near(
            tbl, queries, keys, ahead[s], behind[s], state, s, n - s, heads
        )
    k4 = hop(behind[-1][0], "up")
    v4 = hop(ahead[-1][1], "down")

    att, lse, delta, ds4, pk, pv = turn(
        tbl, queries, grad_out, ot, keys, k4, v4, state, opposite, heads
    )
    stats = (lse, delta)

    def plus(part, x):
        return part if x is None else part + x.astype(jnp.float32)

    k_up, k_down = hop(pk, "up"), None
    v_up, v_down = None, hop(pv, "down")
    gq = None
    for s in range(steps, 0, -1):
        pka, pva, pkb, pvb, gq = back(
            tbl, queries, grad_out, keys, stats, ahead[s], behind[s], gq, s, n - s, heads
        )
        k_up = hop(plus(pka, k_up).astype(jnp.bfloat16), "up")
        k_down = hop(plus(pkb, k_down).astype(jnp.bfloat16), "down")
        v_up = hop(plus(pva, v_up).astype(jnp.bfloat16), "up")
        v_down = hop(plus(pvb, v_down).astype(jnp.bfloat16), "down")
    attended, grad_q, pk, pv = own(
        tbl, queries, grad_out, keys, values, stats, k4, ds4, att, gq, opposite, heads
    )
    grad_k, grad_v = finish(pk, k_up, k_down, pv, v_up, v_down)
    return attended, grad_q, grad_k, grad_v


def solution(mesh):
    spec = P("ctx", "head")
    return jax.shard_map(
        local,
        mesh=mesh,
        in_specs=(spec, spec, spec, spec, P(), P()),
        out_specs=(spec,) * 4,
        check_vma=False,
    )
```

```python
import functools
import math

import jax
import jax.numpy as jnp
from jax import lax
from jax.experimental import pallas as pl
from jax.experimental.pallas import tpu as pltpu
from jax.sharding import PartitionSpec as P


QH = 64
KVH = 8
DH = 128
BLOCK = 128
GROUP = QH // KVH
ROWS = GROUP * BLOCK
SUB = 8

SCALE = 1.0 / math.sqrt(DH)
EXP2_SCALE = SCALE * math.log2(math.e)
VMEM_BYTES = 16 * 1024 * 1024
KEPT = 3
FIRST_PART = 1024
NEAR_PART = 1024
TURN_PART = 1024
BACK_PART = 1024

NT = (((1,), (1,)), ((), ()))
VMEM = pl.BlockSpec(memory_space=pltpu.VMEM)
SMEM = pl.BlockSpec(memory_space=pltpu.SMEM)
HBM = pl.BlockSpec(memory_space=pltpu.HBM)


def dot(a, b):
    return jnp.dot(a, b, preferred_element_type=jnp.float32)


def dot_t(a, b):
    return lax.dot_general(a, b, NT, preferred_element_type=jnp.float32)


def bf16(shape):
    return jax.ShapeDtypeStruct(shape, jnp.bfloat16)


def f32(shape):
    return jax.ShapeDtypeStruct(shape, jnp.float32)


def call(kernel, in_specs, out_shape, flops, args, scratch=(), out_specs=None, size=1 << 20):
    return pl.pallas_call(
        kernel,
        in_specs=in_specs,
        out_specs=out_specs or [VMEM] * len(out_shape),
        out_shape=out_shape,
        scratch_shapes=list(scratch),
        compiler_params=pltpu.CompilerParams(vmem_limit_bytes=VMEM_BYTES),
        cost_estimate=pl.CostEstimate(
            flops=int(flops), bytes_accessed=size, transcendentals=0
        ),
    )(*args)


def at(index, size):
    if isinstance(index, int):
        return pl.ds(index * size, size)
    return pl.ds(pl.multiple_of(index * size, size), size)


def block(ref, i, h):
    return ref[i * BLOCK : (i + 1) * BLOCK, h * DH : (h + 1) * DH]


def tall(tile):
    return jnp.concatenate([tile] * (BLOCK // tile.shape[0]), axis=0)


class Pick:
    def __init__(self, table_ref, j, b):
        self.count = table_ref.shape[2] - 1
        self.tiles = [table_ref[j, b, i] for i in range(self.count + 1)]

    def listed(self, ref, h):
        terms = [block(ref, i, h) * tall(self.tiles[i]) for i in range(self.count)]
        return functools.reduce(jnp.add, terms)

    def key(self, ref, h, own):
        return self.listed(ref, h) + own * tall(self.tiles[self.count])

    def value_t(self, v):
        return jnp.concatenate([v.T, functools.reduce(jnp.add, self.tiles[: self.count])], axis=0)

    def add(self, ref, h, x):
        for i in range(self.count):
            factor = tall(self.tiles[i].astype(jnp.float32))
            ref[i * BLOCK : (i + 1) * BLOCK, h * DH : (h + 1) * DH] += x * factor


def queries_of(ref, b, h, part):
    members = range(part.start // BLOCK, part.stop // BLOCK)
    return jnp.concatenate(
        [ref[at(b, BLOCK), at(h * GROUP + g, DH)] for g in members], axis=0
    )


def split(x):
    return x.reshape(x.shape[0] // SUB, SUB, x.shape[1])


def join(x):
    return x.reshape(x.shape[0] * SUB, x.shape[2])


def all_equal(x):
    return jnp.broadcast_to(jnp.sum(x, axis=0, keepdims=True), x.shape)


def largest(x):
    top = jnp.max(x, axis=0)
    return jnp.broadcast_to(jnp.max(top, axis=0, keepdims=True), top.shape)


def parts(size):
    return [slice(t, t + size) for t in range(0, ROWS, size)]


def staggered(combos, size, phases):
    waiting = [phases(c, part) for c in range(combos) for part in parts(size)]
    active = []
    while waiting or active:
        if waiting:
            active.append(waiting.pop(0))
        active = [g for g in active if next(g, "end") != "end"]


def eye(size):
    row = lax.broadcasted_iota(jnp.int32, (size, size), 0)
    return jnp.where(row == lax.broadcasted_iota(jnp.int32, (size, size), 1), 1.0, 0.0).astype(
        jnp.bfloat16
    )


def unit_kernel(out_ref):
    out_ref[...] = eye(out_ref.shape[0])


def identity():
    return call(unit_kernel, [], [bf16((2 * BLOCK, 2 * BLOCK))], 1e11, (), size=1 << 28)[0]


def table_kernel(slots_ref, counts_ref, out_ref, tbl):
    blk_dev, n = tbl.shape
    me = lax.axis_index("ctx")

    def place(index):
        half = lax.shift_right_logical(index, 1)
        return jnp.where(lax.bitwise_and(index, 1) == 0, half, n - 1 - half)

    for b in range(blk_dev):
        for j in range(n):
            tbl[b, j] = blk_dev
        row = me * blk_dev + b
        for s in range(slots_ref.shape[0]):
            listed = slots_ref[s, row]
            owner = lax.div(listed, blk_dev)
            offset = lax.rem(place(owner) - place(me) + n, n)

            @pl.when(s < counts_ref[row])
            def _():
                tbl[b, offset] = listed - owner * blk_dev

        for j in range(n):
            for i in range(blk_dev + 1):
                value = jnp.where(tbl[b, j] == i, 1.0, 0.0)
                out_ref[j, b, i] = jnp.full((2 * SUB, DH), value, jnp.float32).astype(jnp.bfloat16)


def table(blocks, counts, blk_dev, n):
    return call(
        table_kernel, [SMEM] * 2, [bf16((n, blk_dev, blk_dev + 1, 2 * SUB, DH))], 1e3,
        (blocks.T, counts), [pltpu.SMEM((blk_dev, n), jnp.int32)], size=1 << 10,
    )[0]


def first_kernel(heads, unit_ref, q_ref, o_ref, k_ref, v_ref, ot_ref, acc_ref, m_ref):
    unit = unit_ref[:DH, :DH]

    def phases(c, part):
        b, h = c // heads, c % heads
        x = dot_t(block(k_ref, b, h), queries_of(q_ref, b, h, part))
        turned = dot_t(unit, queries_of(o_ref, b, h, part))
        yield
        v = block(v_ref, b, h).T
        v = jnp.concatenate([v, jnp.ones((2 * SUB, BLOCK), v.dtype)], axis=0)
        x = split(x * EXP2_SCALE)
        m = largest(x)
        m_ref[c, :, part] = m
        p = join(jnp.exp2(x - m)).astype(jnp.bfloat16)
        ot_ref[c, :, part] = turned.astype(jnp.bfloat16)
        yield
        acc_ref[c, :, part] = dot(v, p)[: DH + SUB]

    staggered(m_ref.shape[0], FIRST_PART, phases)


def first(unit, q, o, k, v, combos, heads):
    return call(
        functools.partial(first_kernel, heads),
        [VMEM] * 5,
        [bf16((combos, DH, ROWS)), f32((combos, DH + SUB, ROWS)), f32((combos, SUB, ROWS))],
        6 * combos * ROWS * BLOCK * DH,
        (unit, q, o, k, v),
    )


def near_kernel(
    heads, ja, jb, tbl, q_ref, o_ref, own_ref, ka_ref, va_ref, kb_ref, vb_ref, acc_in, m_in,
    acc_ref, m_ref, *kept,
):
    def phases(c, part):
        b, h = c // heads, c % heads
        pa, pb = Pick(tbl, ja, b), Pick(tbl, jb, b)
        own = block(own_ref, b, h)
        k = jnp.concatenate([pa.key(ka_ref, h, own), pb.key(kb_ref, h, own)], axis=0)
        x = dot_t(k, queries_of(q_ref, b, h, part))
        yield
        va, vb = pa.listed(va_ref, h), pb.listed(vb_ref, h)
        v = jnp.concatenate([pa.value_t(va), pb.value_t(vb)], axis=1)
        x = x * EXP2_SCALE
        if kept:
            kept[0][c, :, part] = x
            kept[1][c, :, part] = dot_t(
                jnp.concatenate([va, vb], axis=0), queries_of(o_ref, b, h, part)
            )
        x = split(x)
        old = m_in[c, :, part]
        m = jnp.maximum(old, largest(x))
        p = join(jnp.exp2(x - m)).astype(jnp.bfloat16)
        m_ref[c, :, part] = m
        yield
        acc = join(split(acc_in[c, :, part]) * jnp.exp2(old - m))
        acc_ref[c, :, part] = acc + dot(v, p)[: DH + SUB]

    staggered(m_ref.shape[0], NEAR_PART, phases)


def near(tbl, q, o, k_own, ahead, behind, state, ja, jb, heads, keep):
    combos = state[1].shape[0]
    kept = [f32((combos, 2 * BLOCK, ROWS))] * 2 if keep else []
    return call(
        functools.partial(near_kernel, heads, ja, jb),
        [VMEM] * 10,
        [f32(a.shape) for a in state] + kept,
        8 * combos * ROWS * BLOCK * DH,
        (tbl, q, o, k_own, *ahead, *behind, *state),
    )


def turn_kernel(
    heads, opposite, tbl, q_ref, o_ref, ot_ref, own_ref, k_ref, v_ref, acc_in, m_in,
    att_ref, lse_ref, delta_ref, ds_ref, pk_ref, pv_ref, pk_scr, pv_scr,
):
    pk_scr[...] = jnp.zeros_like(pk_scr)
    pv_scr[...] = jnp.zeros_like(pv_scr)

    def phases(c, part):
        b, h = c // heads, c % heads
        pick = Pick(tbl, opposite, b)
        k = pick.key(k_ref, h, block(own_ref, b, h))
        v = pick.listed(v_ref, h)
        q, o = queries_of(q_ref, b, h, part), queries_of(o_ref, b, h, part)
        x = dot_t(k, q)
        yield
        grad_p = split(dot_t(v, o))
        v_t = pick.value_t(v)
        x = split(x * EXP2_SCALE)
        old = m_in[c, :, part]
        m = jnp.maximum(old, largest(x))
        p = jnp.exp2(x - m)
        rounded = join(p).astype(jnp.bfloat16)
        yield
        acc = dot(v_t, rounded)[: DH + SUB]
        yield
        acc = split(acc_in[c, :, part]) * jnp.exp2(old - m) + split(acc)
        total = acc[DH // SUB]
        inverse = 1.0 / total
        att = join(acc[: DH // SUB] * inverse).astype(jnp.bfloat16)
        att_ref[c, :, part] = att
        terms = att.astype(jnp.float32) * ot_ref[c, :, part].astype(jnp.float32)
        delta = all_equal(jnp.sum(split(terms), axis=0))
        p = p * inverse
        weights = join(p).astype(jnp.bfloat16)
        ds = join(p * (grad_p - delta)).astype(jnp.bfloat16)
        ds_ref[c, :, part] = ds
        lse_ref[c, :, part] = m + jnp.log2(total)
        delta_ref[c, :, part] = delta
        yield
        pick.add(pk_scr, h, dot(ds, q))
        pick.add(pv_scr, h, dot(weights, o))

    staggered(m_in.shape[0], TURN_PART, phases)
    pk_ref[...] = pk_scr[...].astype(jnp.bfloat16)
    pv_ref[...] = pv_scr[...].astype(jnp.bfloat16)


def turn(tbl, q, o, ot, k_own, k4, v4, state, opposite, heads):
    combos = ot.shape[0]
    return call(
        functools.partial(turn_kernel, heads, opposite),
        [VMEM] * 9,
        [bf16(ot.shape)]
        + [f32((combos, SUB, ROWS))] * 2
        + [bf16((combos, BLOCK, ROWS))]
        + [bf16(k4.shape)] * 2,
        10 * combos * ROWS * BLOCK * DH,
        (tbl, q, o, ot, k_own, k4, v4, *state),
        [pltpu.VMEM(k4.shape, jnp.float32)] * 2,
    )


def weights_and_grads(c, part, x, grad_p, lse_ref, delta_ref):
    p = jnp.exp2(split(x) - lse_ref[c, :, part])
    ds = p * (split(grad_p) - delta_ref[c, :, part])
    return join(p).astype(jnp.bfloat16), join(ds).astype(jnp.bfloat16)


def back_kernel(
    heads, ja, jb, has_sum, has_scores, tbl, q_ref, o_ref, own_ref, lse_ref, delta_ref, ka_ref, va_ref,
    kb_ref, vb_ref, *refs,
):
    if has_sum:
        gq_in, *refs = refs
    if has_scores:
        x_ref, grad_p_ref, *refs = refs
    pka_ref, pva_ref, pkb_ref, pvb_ref, gq_ref = refs
    for ref in (pka_ref, pva_ref, pkb_ref, pvb_ref):
        ref[...] = jnp.zeros_like(ref)

    def phases(c, part):
        b, h = c // heads, c % heads
        pa, pb = Pick(tbl, ja, b), Pick(tbl, jb, b)
        own = block(own_ref, b, h)
        k = jnp.concatenate([pa.key(ka_ref, h, own), pb.key(kb_ref, h, own)], axis=0)
        v = jnp.concatenate([pa.listed(va_ref, h), pb.listed(vb_ref, h)], axis=0)
        q, o = queries_of(q_ref, b, h, part), queries_of(o_ref, b, h, part)
        if has_scores:
            x, grad_p = x_ref[c, :, part], grad_p_ref[c, :, part]
        else:
            x, grad_p = dot_t(k, q) * EXP2_SCALE, dot_t(v, o)
            yield
        weights, ds = weights_and_grads(c, part, x, grad_p, lse_ref, delta_ref)
        yield
        dk, dv = dot(ds, q), dot(weights, o)
        for i, (pick, rk, rv) in enumerate(((pa, pka_ref, pva_ref), (pb, pkb_ref, pvb_ref))):
            src = slice(i * BLOCK, (i + 1) * BLOCK)
            pick.add(rk, h, dk[src])
            pick.add(rv, h, dv[src])
        used = jnp.concatenate([pa.listed(ka_ref, h).T, pb.listed(kb_ref, h).T], axis=1)
        grad = dot(used, ds)
        gq_ref[c, :, part] = gq_in[c, :, part] + grad if has_sum else grad

    staggered(gq_ref.shape[0], BACK_PART, phases)


def back(tbl, q, o, k_own, stats, ahead, behind, gq, scores, ja, jb, heads):
    combos = stats[0].shape[0]
    extra = (() if gq is None else (gq,)) + tuple(scores)
    return call(
        functools.partial(back_kernel, heads, ja, jb, gq is not None, len(scores) > 0),
        [VMEM] * (10 + len(extra)),
        [f32(k_own.shape)] * 4 + [f32((combos, DH, ROWS))],
        20 * combos * ROWS * BLOCK * DH,
        (tbl, q, o, k_own, *stats, *ahead, *behind, *extra),
    )


def own_kernel(
    heads, opposite, tbl, unit_ref, q_ref, o_ref, k_ref, v_ref, lse_ref, delta_ref, k4_ref, ds4_ref,
    att_ref, gq_in, att_out, gq_out, pk_ref, pv_ref, att_scr, gq_scr, sems,
):
    combos = gq_in.shape[0]
    unit = unit_ref[...]

    def send(ref, out, c, kind):
        b, h = c // heads, c % heads
        place = (at(b, BLOCK), at(h, GROUP * DH))
        return pltpu.make_async_copy(ref.at[place], out.at[place], sems.at[kind, c])

    def put(ref, b, h, x):
        for i in range(GROUP // 2):
            y = dot_t(unit, x[:, i * 2 * BLOCK : (i + 1) * 2 * BLOCK]).astype(jnp.bfloat16)
            for j in range(2):
                place = (at(b, BLOCK), at(h * GROUP + 2 * i + j, DH))
                ref[place] = y[j * BLOCK : (j + 1) * BLOCK]

    def phases(c, part):
        b, h = c // heads, c % heads
        q, o = queries_of(q_ref, b, h, part), queries_of(o_ref, b, h, part)
        k = block(k_ref, b, h)
        x, grad_p = dot_t(k, q) * EXP2_SCALE, dot_t(block(v_ref, b, h), o)
        yield
        weights, ds = weights_and_grads(c, part, x, grad_p, lse_ref, delta_ref)
        put(att_scr, b, h, att_ref[c])
        send(att_scr, att_out, c, 0).start()
        yield
        place = (at(b, BLOCK), at(h, DH))
        pk_ref[place] = dot(ds, q)
        pv_ref[place] = dot(weights, o)
        used = jnp.concatenate([k.T, Pick(tbl, opposite, b).listed(k4_ref, h).T], axis=1)
        grad = (gq_in[c] + dot(used, jnp.concatenate([ds, ds4_ref[c]], axis=0))) * SCALE
        yield
        put(gq_scr, b, h, grad.astype(jnp.bfloat16))
        send(gq_scr, gq_out, c, 1).start()

    staggered(combos, ROWS, phases)
    for c in range(combos):
        send(att_scr, att_out, c, 0).wait()
        send(gq_scr, gq_out, c, 1).wait()


def own(tbl, unit, q, o, k, v, stats, k4, ds4, att, gq, opposite, heads):
    combos = gq.shape[0]
    return call(
        functools.partial(own_kernel, heads, opposite),
        [VMEM] * 12,
        [bf16(q.shape), bf16(q.shape), f32(k.shape), f32(k.shape)],
        12 * combos * ROWS * BLOCK * DH,
        (tbl, unit, q, o, k, v, *stats, k4, ds4, att, gq),
        [pltpu.VMEM(q.shape, jnp.bfloat16)] * 2
        + [pltpu.SemaphoreType.DMA((2, combos))],
        [HBM, HBM, VMEM, VMEM],
    )


def finish_kernel(pk_ref, ka_ref, kb_ref, pv_ref, va_ref, vb_ref, gk_ref, gv_ref):
    def total(own, a, b):
        return own[...] + (a[...].astype(jnp.float32) + b[...].astype(jnp.float32))

    gk_ref[...] = (total(pk_ref, ka_ref, kb_ref) * SCALE).astype(jnp.bfloat16)
    gv_ref[...] = total(pv_ref, va_ref, vb_ref).astype(jnp.bfloat16)


def finish(*args):
    return call(finish_kernel, [VMEM] * 6, [bf16(args[0].shape)] * 2, 1e7, args)


def local(queries, keys, values, grad_out, key_blocks, key_count):
    n = lax.axis_size("ctx")
    row_count, width = keys.shape
    blk_dev = row_count // BLOCK
    heads = width // DH
    combos = blk_dev * heads
    opposite = n // 2
    steps = opposite - 1

    order = list(range(0, n, 2)) + list(range(n - 1, 0, -2))
    up = [(order[i], order[(i + 1) % n]) for i in range(n)]
    ways = {"up": up, "down": [(b, a) for a, b in up]}

    def hop(x, way):
        return lax.ppermute(x, "ctx", ways[way])

    behind, ahead = [(keys, values)], [(keys, values)]
    unit = identity()
    tbl = table(key_blocks, key_count, blk_dev, n)
    ot, *state = first(unit, queries, grad_out, keys, values, combos, heads)
    kept, scores = range(max(1, steps + 1 - KEPT), steps + 1), {}
    for s in range(1, steps + 1):
        k_up = hop(behind[-1][0], "up")
        k_down = hop(ahead[-1][0], "down")
        v_up = hop(behind[-1][1], "up")
        v_down = hop(ahead[-1][1], "down")
        behind.append((k_up, v_up))
        ahead.append((k_down, v_down))
        state = near(
            tbl, queries, grad_out, keys, ahead[s], behind[s], state, s, n - s, heads, s in kept
        )
        state, scores[s] = state[:2], state[2:]
    k4 = hop(behind[-1][0], "up")
    v4 = hop(ahead[-1][1], "down")

    att, lse, delta, ds4, pk, pv = turn(
        tbl, queries, grad_out, ot, keys, k4, v4, state, opposite, heads
    )
    stats = (lse, delta)

    def plus(part, x):
        return part if x is None else part + x.astype(jnp.float32)

    k_up, k_down = hop(pk, "up"), None
    v_up, v_down = None, hop(pv, "down")
    gq = None
    for s in range(steps, 0, -1):
        pka, pva, pkb, pvb, gq = back(
            tbl, queries, grad_out, keys, stats, ahead[s], behind[s], gq,
            scores[s], s, n - s, heads,
        )
        k_up = hop(plus(pka, k_up).astype(jnp.bfloat16), "up")
        k_down = hop(plus(pkb, k_down).astype(jnp.bfloat16), "down")
        v_up = hop(plus(pva, v_up).astype(jnp.bfloat16), "up")
        v_down = hop(plus(pvb, v_down).astype(jnp.bfloat16), "down")
    attended, grad_q, pk, pv = own(
        tbl, unit, queries, grad_out, keys, values, stats, k4, ds4, att, gq, opposite, heads
    )
    grad_k, grad_v = finish(pk, k_up, k_down, pv, v_up, v_down)
    return attended, grad_q, grad_k, grad_v


def solution(mesh):
    spec = P("ctx", "head")
    return jax.shard_map(
        local,
        mesh=mesh,
        in_specs=(spec, spec, spec, spec, P(), P()),
        out_specs=(spec,) * 4,
        check_vma=False,
    )
```
